32 devices in a mesh: space: 16 (over z, y, x), tm: 2 (over core).
Axes of the slice: x: 2, y: 2, z: 4, core: 2. Of those that a mesh axis runs over, the one named last changes fastest.
Arguments:
- vectors: bfloat16 [2, 64, 2, 12, 2048], P('tm', None, None, None, 'space'), may hold values from -6 to 6
- dilution: int32 [64], replicated, may hold values from 0 to 23
- gamma_ids: int32 [16], replicated, may hold values from 1 to 15
Outputs:
- gram: float32 [2, 1024, 128], P(None, 'space')
- loops: float32 [2, 1024, 2], P(None, 'space')
The draws below stay inside these ranges and needn't reach their ends.
All inputs are finite; a program needn't handle non-finite values.
Results may differ from the reference program's by a relative error of at most 0.0003.
Values sent between devices are 32-bit elements; how exact they have to be, the bound alone decides.
No kernel may reach another device: no remote copies, remote signals or barrier semaphores. Data moves between devices by JAX's collectives and lax.ppermute only.
A program may use at most 64 MiB of HBM per device.

```python
import math
from functools import partial
import jax
import jax.numpy as jnp
from jax import lax

NVEC = 64
NG = 16
TDIL = 2
NSITES = 2048
NT = 2


def touch_ends(result, rng, least, largest):
    shape = result.shape
    place = [jax.random.randint(jax.random.fold_in(rng, axis), (), 0, shape[axis]) for axis in range(len(shape))]
    result = result.at[tuple(place)].set(least)
    longest = shape.index(max(shape))
    place[longest] = (place[longest] + 1) % shape[longest]
    return result.at[tuple(place)].set(largest)


def level_of(own_key, extent, shards, smallest, largest):
    def one(dim, parts):
        steps = jax.random.uniform(jax.random.fold_in(jax.random.fold_in(own_key, 6), dim), (parts,), jnp.float32, smallest / len(shards), largest / len(shards))
        return jnp.repeat(jnp.exp(steps), extent[dim] // parts).reshape((-1,) + (1,) * (len(extent) - dim - 1))

    factor_of = one(*shards[0])
    for cut in shards[1:]:
        factor_of = factor_of * one(*cut)
    return factor_of


def noise(rng, dims, spread, bound, pieces=(), held_as=jnp.bfloat16):
    result = spread * jax.random.normal(rng, dims, jnp.float32)
    if pieces:
        result = result * level_of(rng, dims, pieces, -0.22, 0.18)
    return jnp.clip(result, -bound, bound).astype(held_as)


def setup_inputs(seed: int = 0) -> dict:
    arg_keys = jax.random.split(jax.random.key(seed), 4)
    return {
        "vectors": noise(arg_keys[0], (NT, NVEC, 2, 12, NSITES), 1.0, 6.0, ((0, 2), (4, 16))),
        "dilution": touch_ends(jax.random.randint(arg_keys[1], (NVEC,), 0, 12 * TDIL), jax.random.fold_in(arg_keys[1], 1), 0, (12 * TDIL) - 1).astype(jnp.int32),
        "gamma_ids": touch_ends(jax.random.randint(arg_keys[2], (NG,), 1, 16), jax.random.fold_in(arg_keys[2], 1), 1, 15).astype(jnp.int32),
    }


highest = lax.Precision.HIGHEST

def zero_square():
    return [[0, 0, 0, 0] for _ in range(4)]

def pair_product(left, right):
    real_out = zero_square()
    imag_out = zero_square()
    for row in range(4):
        for col in range(4):
            acc_real = 0
            acc_imag = 0
            for mid in range(4):
                acc_real += left[0][row][mid] * right[0][mid][col] - left[1][row][mid] * right[1][mid][col]
                acc_imag += left[0][row][mid] * right[1][mid][col] + left[1][row][mid] * right[0][mid][col]
            real_out[row][col] = acc_real
            imag_out[row][col] = acc_imag
    return (real_out, imag_out)

def dirac_tables():
    factors = [(zero_square(), [[0, 0, 0, 1], [0, 0, 1, 0], [0, -1, 0, 0], [-1, 0, 0, 0]]), ([[0, 0, 0, -1], [0, 0, 1, 0], [0, 1, 0, 0], [-1, 0, 0, 0]], zero_square()), (zero_square(), [[0, 0, 1, 0], [0, 0, 0, -1], [-1, 0, 0, 0], [0, 1, 0, 0]]), ([[0, 0, 1, 0], [0, 0, 0, 1], [1, 0, 0, 0], [0, 1, 0, 0]], zero_square())]
    reals = []
    imags = []
    for number in range(16):
        current = ([[1 if a == b else 0 for b in range(4)] for a in range(4)], zero_square())
        for position in range(4):
            if number >> position & 1:
                current = pair_product(current, factors[position])
        reals.append([value for line in current[0] for value in line])
        imags.append([value for line in current[1] for value in line])
    return (reals, imags)

def pick_gammas(gamma_ids):
    table_real, table_imag = dirac_tables()
    choose = (gamma_ids[:, None] == jnp.arange(16, dtype=jnp.int32)[None, :]).astype(jnp.float32)
    gamma_real = jnp.dot(choose, jnp.asarray(table_real, dtype=jnp.float32), precision=highest).reshape(-1, 4, 4)
    gamma_imag = jnp.dot(choose, jnp.asarray(table_imag, dtype=jnp.float32), precision=highest).reshape(-1, 4, 4)
    return (gamma_real, gamma_imag)

def reference(vectors, dilution, gamma_ids):
    times, count, halves, comps, sites = vectors.shape
    gamma_real, gamma_imag = pick_gammas(gamma_ids)
    gram_scale = 1.0 / math.sqrt(48.0 * sites)
    loop_scale = 1.0 / math.sqrt(1.0 * sites)
    spin_pick = ((dilution % 12 // 3)[:, None] == jnp.arange(4, dtype=jnp.int32)[None, :]).astype(jnp.float32)
    colour_pick = ((dilution % 3)[:, None] == jnp.arange(3, dtype=jnp.int32)[None, :]).astype(jnp.float32)
    time_class = dilution // 12
    ein = partial(jnp.einsum, precision=highest)

    def one_slice(inputs):
        block, slice_index = inputs
        field = block.astype(jnp.float32).reshape(count, 2, 4, 3, sites)
        real_part = field[:, 0]
        imag_part = field[:, 1]
        pair_real = ein('iack,jbck->iajb', real_part, real_part) + ein('iack,jbck->iajb', imag_part, imag_part)
        pair_imag = ein('iack,jbck->iajb', real_part, imag_part) - ein('iack,jbck->iajb', imag_part, real_part)
        gram_real = ein('gab,iajb->gij', gamma_real, pair_real) - ein('gab,iajb->gij', gamma_imag, pair_imag)
        gram_imag = ein('gab,iajb->gij', gamma_real, pair_imag) + ein('gab,iajb->gij', gamma_imag, pair_real)
        gram = jnp.concatenate([gram_real, gram_imag], axis=2).reshape(-1, 2 * count) * gram_scale
        site_sums = lax.optimization_barrier(jnp.sum(field, axis=-1))
        picked = ein('ipac,ic->ipa', site_sums, colour_pick)
        rows_real = ein('gba,ib->gia', gamma_real, spin_pick)
        rows_imag = ein('gba,ib->gia', gamma_imag, spin_pick)
        loop_real = ein('gia,ia->gi', rows_real, picked[:, 0]) - ein('gia,ia->gi', rows_imag, picked[:, 1])
        loop_imag = ein('gia,ia->gi', rows_real, picked[:, 1]) + ein('gia,ia->gi', rows_imag, picked[:, 0])
        live = (time_class == slice_index % TDIL).astype(jnp.float32)[None, :]
        loops = jnp.stack([loop_real * live, loop_imag * live], axis=-1).reshape(-1, 2) * loop_scale
        return (gram, loops)
    gram, loops = lax.map(one_slice, (vectors, jnp.arange(times, dtype=jnp.int32)))
    return (gram, loops)
```

```python
from functools import partial
import math

import jax
import jax.numpy as jnp
from jax import lax
from jax.experimental import pallas as pl
from jax.experimental.pallas import tpu as pltpu
from jax.sharding import PartitionSpec as P

TDIL = 2
SPINS = 4
COLOURS = 3
LANES = 128

EXCHANGE_ORDER = (9, 8, 0, 10, 15, 4, 1, 7, 5, 2, 11, 12, 6, 3, 13, 14)


highest = lax.Precision.HIGHEST


def zero_square():
    return [[0, 0, 0, 0] for _ in range(4)]


def pair_product(left, right):
    real_out = zero_square()
    imag_out = zero_square()
    for row in range(4):
        for col in range(4):
            acc_real = 0
            acc_imag = 0
            for mid in range(4):
                acc_real += (
                    left[0][row][mid] * right[0][mid][col] - left[1][row][mid] * right[1][mid][col]
                )
                acc_imag += (
                    left[0][row][mid] * right[1][mid][col] + left[1][row][mid] * right[0][mid][col]
                )
            real_out[row][col] = acc_real
            imag_out[row][col] = acc_imag
    return (real_out, imag_out)


def dirac_squares():
    factors = [
        (zero_square(), [[0, 0, 0, 1], [0, 0, 1, 0], [0, -1, 0, 0], [-1, 0, 0, 0]]),
        ([[0, 0, 0, -1], [0, 0, 1, 0], [0, 1, 0, 0], [-1, 0, 0, 0]], zero_square()),
        (zero_square(), [[0, 0, 1, 0], [0, 0, 0, -1], [-1, 0, 0, 0], [0, 1, 0, 0]]),
        ([[0, 0, 1, 0], [0, 0, 0, 1], [1, 0, 0, 0], [0, 1, 0, 0]], zero_square()),
    ]
    squares = []
    for number in range(16):
        current = ([[1 if a == b else 0 for b in range(4)] for a in range(4)], zero_square())
        for position in range(4):
            if number >> position & 1:
                current = pair_product(current, factors[position])
        squares.append(current)
    return squares


def dirac_bits():
    imaginary, anti, mask_low, mask_high = 0, 0, 0, 0
    negative = [0, 0, 0, 0]
    for number, (real, imag) in enumerate(dirac_squares()):
        places = [[b for b in range(4) if real[a][b] or imag[a][b]] for a in range(4)]
        mask = places[0][0]
        assert all(places[a] == [a ^ mask] for a in range(4))
        kind = int(imag[0][mask] != 0)
        values = [(imag if kind else real)[a][a ^ mask] for a in range(4)]
        assert all(abs(v) == 1 for v in values)
        sign = -1 if kind else 1
        flips = {values[a] * values[a ^ mask] * sign for a in range(4)}
        assert len(flips) == 1
        imaginary |= kind << number
        anti |= int(flips == {-1}) << number
        mask_low |= (mask & 1) << number
        mask_high |= (mask >> 1) << number
        for a in range(4):
            negative[a] |= int(values[a] < 0) << number
    return imaginary, anti, mask_low, mask_high, negative


IMAGINARY, ANTI, MASK_LOW, MASK_HIGH, NEGATIVE = dirac_bits()


def bit(word, number):
    return (jnp.int32(word) >> number) & 1


def pick_gammas(gamma_ids):
    squares = dirac_squares()
    table_real = [[v for line in real for v in line] for real, _ in squares]
    table_imag = [[v for line in imag for v in line] for _, imag in squares]
    choose = (gamma_ids[:, None] == jnp.arange(16, dtype=jnp.int32)[None, :]).astype(jnp.float32)
    gamma_real = jnp.dot(
        choose, jnp.asarray(table_real, dtype=jnp.float32), precision=highest
    ).reshape(-1, 4, 4)
    gamma_imag = jnp.dot(
        choose, jnp.asarray(table_imag, dtype=jnp.float32), precision=highest
    ).reshape(-1, 4, 4)
    return (gamma_real, gamma_imag)


def half_swap(value, count):
    return pltpu.roll(value, count, 1)


def partial_kernel(
    count, order, ids_ref, dilution_ref, block_ref, out_ref, flat_ref, left_ref, right_ref, pair_ref, loop_ref
):
    comps = SPINS * COLOURS
    width = COLOURS * LANES
    rows = count // 2
    flat_ref[...] = block_ref[...].astype(jnp.float32)
    for spin in range(SPINS):
        for part in range(2):
            for colour in range(COLOURS):
                start = (spin * COLOURS + colour) * 2 + part
                piece = flat_ref[pl.ds(start, count, stride=2 * comps), :]
                here = pl.ds(spin * count, count)
                lanes = pl.ds(part * width + colour * LANES, LANES)
                other = pl.ds((1 - part) * width + colour * LANES, LANES)
                left_ref[here, lanes] = piece.astype(jnp.bfloat16)
                right_ref[here, other] = (piece if part else -piece).astype(jnp.bfloat16)
    total = SPINS * count
    row_id = lax.broadcasted_iota(jnp.int32, (16, 2 * width), 0)
    lane_id = lax.broadcasted_iota(jnp.int32, (16, 2 * width), 1)
    ones = jnp.where(lane_id // LANES == row_id, 1.0, 0.0) * jnp.where(row_id < COLOURS, 1.0, 0.0)
    left_ref[pl.ds(total, 16), :] = ones.astype(jnp.bfloat16)
    dims = (((1,), (1,)), ((), ()))
    real = lax.dot_general(
        left_ref[...], left_ref[pl.ds(0, total), :], dims, preferred_element_type=jnp.float32
    )
    imag = lax.dot_general(left_ref[...], right_ref[...], dims, preferred_element_type=jnp.float32)
    columns = total // LANES
    for spin in range(SPINS):
        for column in range(columns):
            r = real[spin * count : (spin + 1) * count, column * LANES : (column + 1) * LANES]
            i = imag[spin * count : (spin + 1) * count, column * LANES : (column + 1) * LANES]
            pair_ref[0, spin, column] = r + i
            pair_ref[1, spin, column] = r - i

    lane = lax.broadcasted_iota(jnp.int32, (1, LANES), 1)
    high = lane >= count
    half = high.astype(jnp.int32)
    index = jnp.concatenate([dilution_ref[...]] * 2, axis=1)
    spin_of = index % comps // COLOURS
    colour_of = index % COLOURS
    sums = []
    for grid in (real, imag):
        for column in range(columns):
            picked = jnp.zeros((1, LANES), jnp.float32)
            for colour in range(COLOURS):
                row = grid[total + colour : total + colour + 1, column * LANES : (column + 1) * LANES]
                picked = jnp.where(colour_of == colour, row, picked)
            sums.append(picked)
    for mask in range(4):
        source = spin_of ^ mask
        found = []
        for part in range(2):
            lower, upper = sums[part * columns], sums[part * columns + 1]
            value = jnp.where(source >= 2, upper, lower)
            value = jnp.where((source & 1) == half, value, 0.0)
            found.append(value + half_swap(value, count))
        loop_ref[0, mask] = jnp.where(high, found[1], found[0])
        loop_ref[1, mask] = jnp.where(high, found[0], -found[1])

    wide_high = lax.broadcasted_iota(jnp.int32, (rows, LANES), 1) >= count
    for place, owner in enumerate(order):
        number = ids_ref[owner]
        imaginary, anti = bit(IMAGINARY, number), bit(ANTI, number)
        low, upper = bit(MASK_LOW, number), bit(MASK_HIGH, number)
        signs = [1 - 2 * bit(NEGATIVE[a], number) for a in range(4)]
        turn = 1 - 2 * (anti & (1 - imaginary))
        kind = imaginary ^ anti
        odd = wide_high.astype(jnp.int32) == low
        halves = []
        for top in range(2):
            here = pl.ds(top * rows, rows)
            gathered = None
            for pair in range(2):
                column = upper ^ pair
                even_sign = (signs[2 * pair] * turn).astype(jnp.float32)
                odd_sign = (signs[2 * pair + 1] * turn).astype(jnp.float32)
                term = jnp.where(
                    odd,
                    even_sign * pair_ref[kind, 2 * pair, column, here, :],
                    odd_sign * pair_ref[kind, 2 * pair + 1, column, here, :],
                )
                gathered = term if gathered is None else gathered + term
            halves.append(gathered)
        kept = jnp.where(wide_high, halves[1], halves[0])
        moved = jnp.where(wide_high, halves[0], halves[1])
        base = place * (rows + 1)
        out_ref[pl.ds(base, rows), :] = kept + half_swap(moved, count)
        sign = jnp.zeros((1, LANES), jnp.int32)
        for a in range(4):
            sign = jnp.where(spin_of == a, signs[a], sign)
        mask = low + 2 * upper
        out_ref[pl.ds(base + rows, 1), :] = sign.astype(jnp.float32) * loop_ref[imaginary, mask]


def sum_kernel(chunks, rows, parts_ref, out_ref):
    total = parts_ref[pl.ds(0, rows), :]
    for chunk in range(1, chunks):
        total = total + parts_ref[pl.ds(chunk * rows, rows), :]
    out_ref[...] = total


def finish_kernel(count, gram_scale, loop_scale, ids_ref, dilution_ref, mine_ref, other_ref, gram_ref, loop_ref):
    rows = count // 2
    own = lax.axis_index("tm")
    number = ids_ref[lax.axis_index("space")]
    anti = bit(ANTI, number)
    high = lax.broadcasted_iota(jnp.int32, (rows, LANES), 1) >= count
    full_high = lax.broadcasted_iota(jnp.int32, (count, LANES), 1) >= count
    time_class = dilution_ref[...] // (SPINS * COLOURS)
    for ref, slice_index in ((mine_ref, own), (other_ref, 1 - own)):
        packed = ref[pl.ds(0, rows), :]
        swapped = half_swap(packed, count)
        square = jnp.concatenate(
            [jnp.where(high, swapped, packed), jnp.where(high, packed, swapped)], axis=0
        )
        turned = jnp.transpose(jnp.concatenate([square, square], axis=0))[:count]
        real = (square + turned) * (0.5 * gram_scale)
        imag = (square - turned) * (0.5 * gram_scale)
        plain = jnp.where(full_high, imag, real)
        rotated = jnp.where(full_high, real, -imag)
        gram_ref[slice_index] = jnp.where(anti == 1, rotated, plain)
        row = ref[pl.ds(rows, 1), :] * loop_scale
        both = jnp.concatenate([row, half_swap(row, count)], axis=0)
        live = (time_class == slice_index % TDIL).astype(jnp.float32)
        loop_ref[slice_index] = both[:, :count] * live


def packed_shards(vectors, dilution, gamma_ids):
    slices, count, halves, comps, sites = vectors.shape
    owners = lax.axis_size("space")
    total_sites = sites * owners
    gram_scale = 1.0 / math.sqrt(48.0 * total_sites)
    loop_scale = 1.0 / math.sqrt(1.0 * total_sites)
    order = EXCHANGE_ORDER if owners == len(EXCHANGE_ORDER) else tuple(range(owners))
    rows = count // 2
    chunk = rows + 1
    block = jnp.transpose(vectors, (0, 1, 3, 2, 4)).reshape(count * comps * halves, sites)
    vmem = pl.BlockSpec(memory_space=pltpu.VMEM)
    smem = pl.BlockSpec(memory_space=pltpu.SMEM)
    total = SPINS * count
    parts = pl.pallas_call(
        partial(partial_kernel, count, order),
        out_shape=jax.ShapeDtypeStruct((owners * chunk, LANES), jnp.float32),
        in_specs=[smem, vmem, vmem],
        out_specs=vmem,
        scratch_shapes=[
            pltpu.VMEM((count * comps * halves, LANES), jnp.float32),
            pltpu.VMEM((total + 16, 2 * COLOURS * LANES), jnp.bfloat16),
            pltpu.VMEM((total, 2 * COLOURS * LANES), jnp.bfloat16),
            pltpu.VMEM((2, SPINS, total // LANES, count, LANES), jnp.float32),
            pltpu.VMEM((2, 4, 1, LANES), jnp.float32),
        ],
        compiler_params=pltpu.CompilerParams(vmem_limit_bytes=16 << 20),
        name="partial_gram",
    )(gamma_ids, dilution.reshape(1, count), block)
    swapped = lax.all_to_all(
        parts.reshape(owners, chunk, 1, LANES),
        "space",
        0,
        0,
        tiled=True,
        axis_index_groups=[list(order)],
    )
    mine = pl.pallas_call(
        partial(sum_kernel, owners, chunk),
        out_shape=jax.ShapeDtypeStruct((chunk, LANES), jnp.float32),
        in_specs=[vmem],
        out_specs=vmem,
        compiler_params=pltpu.CompilerParams(vmem_limit_bytes=4 << 20),
        name="sum_chunks",
    )(swapped.reshape(owners * chunk, LANES))
    other = lax.ppermute(mine, "tm", [(0, 1), (1, 0)])
    gram, loops = pl.pallas_call(
        partial(finish_kernel, count, gram_scale, loop_scale),
        out_shape=(
            jax.ShapeDtypeStruct((2, count, LANES), jnp.float32),
            jax.ShapeDtypeStruct((2, 2, count), jnp.float32),
        ),
        in_specs=[smem, vmem, vmem, vmem],
        out_specs=(vmem, vmem),
        compiler_params=pltpu.CompilerParams(vmem_limit_bytes=4 << 20),
        name="finish",
    )(gamma_ids, dilution.reshape(1, count), mine, other)
    return gram, jnp.transpose(loops, (0, 2, 1))


def general_shards(vectors, dilution, gamma_ids):
    slices, count, halves, comps, sites = vectors.shape
    owners = lax.axis_size("space")
    total_sites = sites * owners
    gram_scale = 1.0 / math.sqrt(48.0 * total_sites)
    loop_scale = 1.0 / math.sqrt(1.0 * total_sites)
    gamma_real, gamma_imag = pick_gammas(gamma_ids)
    spin_pick = ((dilution % 12 // 3)[:, None] == jnp.arange(4, dtype=jnp.int32)[None, :]).astype(
        jnp.float32
    )
    colour_pick = ((dilution % 3)[:, None] == jnp.arange(3, dtype=jnp.int32)[None, :]).astype(
        jnp.float32
    )
    time_class = dilution // 12
    ein = partial(jnp.einsum, precision=highest)
    lowein = partial(jnp.einsum, preferred_element_type=jnp.float32)
    first_slice = lax.axis_index("tm") * slices
    rows_real = ein("gba,ib->gia", gamma_real, spin_pick)
    rows_imag = ein("gba,ib->gia", gamma_imag, spin_pick)

    def one_slice(inputs):
        block, slice_index = inputs
        spinor = block.reshape(count, 2, 4, 3 * sites)
        real_part = spinor[:, 0]
        imag_part = spinor[:, 1]
        pair_real = lowein("iak,jbk->iajb", real_part, real_part) + lowein(
            "iak,jbk->iajb", imag_part, imag_part
        )
        pair_imag = lowein("iak,jbk->iajb", real_part, imag_part) - lowein(
            "iak,jbk->iajb", imag_part, real_part
        )
        gram_real = ein("gab,iajb->gij", gamma_real, pair_real) - ein(
            "gab,iajb->gij", gamma_imag, pair_imag
        )
        gram_imag = ein("gab,iajb->gij", gamma_real, pair_imag) + ein(
            "gab,iajb->gij", gamma_imag, pair_real
        )
        gram = jnp.concatenate([gram_real, gram_imag], axis=2).reshape(-1, 2 * count)
        gram = gram * gram_scale
        site_sums = jnp.sum(block, axis=-1, dtype=jnp.float32).reshape(count, 2, 4, 3)
        picked = ein("ipac,ic->ipa", site_sums, colour_pick)
        loop_real = ein("gia,ia->gi", rows_real, picked[:, 0]) - ein(
            "gia,ia->gi", rows_imag, picked[:, 1]
        )
        loop_imag = ein("gia,ia->gi", rows_real, picked[:, 1]) + ein(
            "gia,ia->gi", rows_imag, picked[:, 0]
        )
        live = (time_class == slice_index % TDIL).astype(jnp.float32)[None, :]
        loops = jnp.stack([loop_real * live, loop_imag * live], axis=-1).reshape(-1, 2) * loop_scale
        return (gram, loops)

    gram_terms, loop_terms = lax.map(
        one_slice, (vectors, first_slice + jnp.arange(slices, dtype=jnp.int32))
    )
    owned = gram_terms.shape[1] // owners
    width = 2 * count
    padded = jnp.pad(loop_terms, ((0, 0), (0, 0), (0, width - 2)))
    terms = jnp.stack([gram_terms, padded], axis=1).reshape(slices * 2, owners, owned, width)
    swapped = lax.all_to_all(terms, "space", 1, 1, tiled=True)
    mine = jnp.sum(swapped, axis=1).reshape(slices, 2, owned, width)
    every = lax.all_gather(mine, "tm", axis=0, tiled=True)
    return (every[:, 0], every[:, 1, :, :2])


def solution(mesh):
    placed = (P("tm", None, None, None, "space"), P(), P())

    def shards(vectors, dilution, gamma_ids):
        slices, count, halves, comps, sites = vectors.shape
        packable = (
            slices == 1
            and mesh.shape["tm"] == 2
            and gamma_ids.shape[0] == mesh.shape["space"]
            and 2 * count == LANES
            and comps == SPINS * COLOURS
            and halves == 2
            and sites == LANES
        )
        body = packed_shards if packable else general_shards
        return body(vectors, dilution, gamma_ids)

    return jax.shard_map(
        shards,
        mesh=mesh,
        in_specs=placed,
        out_specs=(P(None, "space", None), P(None, "space", None)),
        check_vma=False,
    )
```

```python
from functools import partial
import math

import jax
import jax.numpy as jnp
from jax import lax
from jax.experimental import pallas as pl
from jax.experimental.pallas import tpu as pltpu
from jax.sharding import PartitionSpec as P

TDIL = 2
SPINS = 4
COLOURS = 3
LANES = 128
PIECES = 4

EXCHANGE_ORDER = (8, 1, 7, 10, 14, 15, 13, 4, 9, 11, 5, 2, 12, 0, 6, 3)


highest = lax.Precision.HIGHEST


def zero_square():
    return [[0, 0, 0, 0] for _ in range(4)]


def pair_product(left, right):
    real_out = zero_square()
    imag_out = zero_square()
    for row in range(4):
        for col in range(4):
            acc_real = 0
            acc_imag = 0
            for mid in range(4):
                acc_real += (
                    left[0][row][mid] * right[0][mid][col] - left[1][row][mid] * right[1][mid][col]
                )
                acc_imag += (
                    left[0][row][mid] * right[1][mid][col] + left[1][row][mid] * right[0][mid][col]
                )
            real_out[row][col] = acc_real
            imag_out[row][col] = acc_imag
    return (real_out, imag_out)


def dirac_squares():
    factors = [
        (zero_square(), [[0, 0, 0, 1], [0, 0, 1, 0], [0, -1, 0, 0], [-1, 0, 0, 0]]),
        ([[0, 0, 0, -1], [0, 0, 1, 0], [0, 1, 0, 0], [-1, 0, 0, 0]], zero_square()),
        (zero_square(), [[0, 0, 1, 0], [0, 0, 0, -1], [-1, 0, 0, 0], [0, 1, 0, 0]]),
        ([[0, 0, 1, 0], [0, 0, 0, 1], [1, 0, 0, 0], [0, 1, 0, 0]], zero_square()),
    ]
    squares = []
    for number in range(16):
        current = ([[1 if a == b else 0 for b in range(4)] for a in range(4)], zero_square())
        for position in range(4):
            if number >> position & 1:
                current = pair_product(current, factors[position])
        squares.append(current)
    return squares


def dirac_bits():
    imaginary, anti, mask_low, mask_high = 0, 0, 0, 0
    negative = [0, 0, 0, 0]
    for number, (real, imag) in enumerate(dirac_squares()):
        places = [[b for b in range(4) if real[a][b] or imag[a][b]] for a in range(4)]
        mask = places[0][0]
        assert all(places[a] == [a ^ mask] for a in range(4))
        kind = int(imag[0][mask] != 0)
        values = [(imag if kind else real)[a][a ^ mask] for a in range(4)]
        assert all(abs(v) == 1 for v in values)
        sign = -1 if kind else 1
        flips = {values[a] * values[a ^ mask] * sign for a in range(4)}
        assert len(flips) == 1
        imaginary |= kind << number
        anti |= int(flips == {-1}) << number
        mask_low |= (mask & 1) << number
        mask_high |= (mask >> 1) << number
        for a in range(4):
            negative[a] |= int(values[a] < 0) << number
    return imaginary, anti, mask_low, mask_high, negative


IMAGINARY, ANTI, MASK_LOW, MASK_HIGH, NEGATIVE = dirac_bits()


def bit(word, number):
    return (jnp.int32(word) >> number) & 1


def pick_gammas(gamma_ids):
    squares = dirac_squares()
    table_real = [[v for line in real for v in line] for real, _ in squares]
    table_imag = [[v for line in imag for v in line] for _, imag in squares]
    choose = (gamma_ids[:, None] == jnp.arange(16, dtype=jnp.int32)[None, :]).astype(jnp.float32)
    gamma_real = jnp.dot(
        choose, jnp.asarray(table_real, dtype=jnp.float32), precision=highest
    ).reshape(-1, 4, 4)
    gamma_imag = jnp.dot(
        choose, jnp.asarray(table_imag, dtype=jnp.float32), precision=highest
    ).reshape(-1, 4, 4)
    return (gamma_real, gamma_imag)


def in_hbm(value):
    return pltpu.with_memory_space_constraint(value, pltpu.HBM)


def half_swap(value, count):
    return pltpu.roll(value, count, 1)


def partial_kernel(
    count, order, loop_scale, ids_hbm, dilution_hbm, block_hbm, out_ref, notes_ref,
    ids_ref, dilution_ref, block_ref, flat_ref, left_ref, right_ref, kept_ref, loop_ref, sems,
):
    comps = SPINS * COLOURS
    width = COLOURS * LANES
    rows = count // 2
    total = SPINS * count
    columns = total // LANES
    pieces = PIECES
    batch = count // pieces
    span = batch * comps * 2
    copies = [
        pltpu.make_async_copy(
            block_hbm.at[pl.ds(piece * span, span), :],
            block_ref.at[pl.ds(piece * span, span), :],
            sems.at[piece],
        )
        for piece in range(pieces)
    ]
    for copy in copies:
        copy.start()
    get_dilution = pltpu.make_async_copy(dilution_hbm, dilution_ref, sems.at[pieces])
    get_ids = pltpu.make_async_copy(ids_hbm, ids_ref, sems.at[pieces + 1])
    get_dilution.start()
    get_ids.start()

    row_id = lax.broadcasted_iota(jnp.int32, (16, 2 * width), 0)
    lane_id = lax.broadcasted_iota(jnp.int32, (16, 2 * width), 1)
    ones = jnp.where((lane_id // LANES == row_id) & (row_id < COLOURS), 1.0, 0.0)
    left_ref[pl.ds(total, 16), :] = ones.astype(jnp.bfloat16)

    for piece in range(pieces):
        copies[piece].wait()
        there = pl.ds(piece * span, span)
        flat_ref[there, :] = block_ref[there, :].astype(jnp.float32)
        for spin in range(SPINS):
            here = pl.ds(spin * count + piece * batch, batch)
            for part in range(2):
                for colour in range(COLOURS):
                    start = piece * span + (spin * COLOURS + colour) * 2 + part
                    value = flat_ref[pl.ds(start, batch, stride=2 * comps), :]
                    lanes = pl.ds(part * width + colour * LANES, LANES)
                    other = pl.ds((1 - part) * width + colour * LANES, LANES)
                    left_ref[here, lanes] = value.astype(jnp.bfloat16)
                    right_ref[here, other] = (value if part else -value).astype(jnp.bfloat16)

    dims = (((1,), (1,)), ((), ()))
    real = lax.dot_general(
        left_ref[...], left_ref[pl.ds(0, total), :], dims, preferred_element_type=jnp.float32
    )
    imag = lax.dot_general(left_ref[...], right_ref[...], dims, preferred_element_type=jnp.float32)

    wide_high = lax.broadcasted_iota(jnp.int32, (rows, LANES), 1) >= count
    for pair in range(2):
        for column in range(columns):
            across = slice(column * LANES, (column + 1) * LANES)
            blocks = []
            for spin in (2 * pair, 2 * pair + 1):
                down = slice(spin * count, (spin + 1) * count)
                r, i = real[down, across], imag[down, across]
                blocks.append((r + i, r - i))
            for kind in range(2):
                even, odd = blocks[0][kind], blocks[1][kind]
                for low in range(2):
                    first, second = (odd, even) if low else (even, odd)
                    kept = jnp.where(wide_high, second[rows:], first[:rows])
                    moved = jnp.where(wide_high, second[:rows], first[rows:])
                    kept_ref[kind, low, pair, column, 0] = kept
                    kept_ref[kind, low, pair, column, 1] = half_swap(moved, count)

    get_dilution.wait()
    lane = lax.broadcasted_iota(jnp.int32, (1, LANES), 1)
    high = lane >= count
    half = high.astype(jnp.int32)
    index = jnp.concatenate([dilution_ref[...]] * 2, axis=1)
    spin_of = index % comps // COLOURS
    colour_of = index % COLOURS
    sums = []
    for grid in (real, imag):
        for column in range(columns):
            picked = jnp.zeros((1, LANES), jnp.float32)
            for colour in range(COLOURS):
                row = grid[total + colour : total + colour + 1, column * LANES : (column + 1) * LANES]
                picked = jnp.where(colour_of == colour, row, picked)
            sums.append(picked)
    for mask in range(4):
        source = spin_of ^ mask
        found = []
        for part in range(2):
            lower, upper = sums[part * columns], sums[part * columns + 1]
            value = jnp.where(source >= 2, upper, lower)
            value = jnp.where((source & 1) == half, value, 0.0)
            found.append(value + half_swap(value, count))
        loop_ref[0, mask] = jnp.where(high, found[1], found[0])
        loop_ref[1, mask] = jnp.where(high, found[0], -found[1])

    get_ids.wait()
    for place, owner in enumerate(order):
        number = ids_ref[owner]
        imaginary, anti = bit(IMAGINARY, number), bit(ANTI, number)
        low, upper = bit(MASK_LOW, number), bit(MASK_HIGH, number)
        signs = [1 - 2 * bit(NEGATIVE[a], number) for a in range(4)]
        turn = 1 - 2 * (anti & (1 - imaginary))
        kind = imaginary ^ anti
        packed = None
        for pair in range(2):
            even, odd = signs[2 * pair] * turn, signs[2 * pair + 1] * turn
            first = jnp.where(low == 1, odd, even).astype(jnp.float32)
            second = jnp.where(low == 1, even, odd).astype(jnp.float32)
            column = upper ^ pair
            term = jnp.where(wide_high, second, first) * kept_ref[kind, low, pair, column, 0]
            term += jnp.where(wide_high, first, second) * kept_ref[kind, low, pair, column, 1]
            packed = term if packed is None else packed + term
        base = place * (rows + 1)
        out_ref[pl.ds(base, rows), :] = packed
        sign = jnp.zeros((1, LANES), jnp.int32)
        for a in range(4):
            sign = jnp.where(spin_of == a, signs[a], sign)
        mask = low + 2 * upper
        out_ref[pl.ds(base + rows, 1), :] = sign.astype(jnp.float32) * loop_ref[imaginary, mask]

    anti = bit(ANTI, ids_ref[lax.axis_index("space")])
    time_class = index // comps
    own = lax.axis_index("tm")
    notes_ref[pl.ds(0, 1), :] = jnp.full((1, LANES), anti, jnp.int32).astype(jnp.float32)
    notes_ref[pl.ds(1, 1), :] = jnp.where(time_class == own % TDIL, loop_scale, 0.0)
    notes_ref[pl.ds(2, 1), :] = jnp.where(time_class == (1 - own) % TDIL, loop_scale, 0.0)


def sum_kernel(chunks, rows, parts_ref, out_ref):
    total = parts_ref[pl.ds(0, rows), :]
    for chunk in range(1, chunks):
        total = total + parts_ref[pl.ds(chunk * rows, rows), :]
    out_ref[...] = total


def finish_kernel(count, gram_scale, notes_ref, mine_ref, other_ref, gram_ref, loop_ref):
    rows = count // 2
    own = lax.axis_index("tm")
    anti = notes_ref[pl.ds(0, 1), :] > 0.5
    high = lax.broadcasted_iota(jnp.int32, (rows, LANES), 1) >= count
    full_high = lax.broadcasted_iota(jnp.int32, (count, LANES), 1) >= count
    for place, (ref, slice_index) in enumerate(((mine_ref, own), (other_ref, 1 - own))):
        packed = ref[pl.ds(0, rows), :]
        swapped = half_swap(packed, count)
        square = jnp.concatenate(
            [jnp.where(high, swapped, packed), jnp.where(high, packed, swapped)], axis=0
        )
        turned = jnp.transpose(jnp.concatenate([square, square], axis=0))[:count]
        real = (square + turned) * (0.5 * gram_scale)
        imag = (square - turned) * (0.5 * gram_scale)
        plain = jnp.where(full_high, imag, real)
        rotated = jnp.where(full_high, real, -imag)
        gram_ref[slice_index] = jnp.where(anti, rotated, plain)
        row = ref[pl.ds(rows, 1), :] * notes_ref[pl.ds(1 + place, 1), :]
        both = jnp.concatenate([row, half_swap(row, count)], axis=0)
        loop_ref[slice_index] = both[:, :count]


def packed_shards(vectors, dilution, gamma_ids):
    slices, count, halves, comps, sites = vectors.shape
    owners = lax.axis_size("space")
    total_sites = sites * owners
    gram_scale = 1.0 / math.sqrt(48.0 * total_sites)
    loop_scale = 1.0 / math.sqrt(1.0 * total_sites)
    order = EXCHANGE_ORDER if owners == len(EXCHANGE_ORDER) else tuple(range(owners))
    rows = count // 2
    chunk = rows + 1
    block = jnp.transpose(vectors, (0, 1, 3, 2, 4)).reshape(count * comps * halves, sites)
    vmem = pl.BlockSpec(memory_space=pltpu.VMEM)
    hbm = pl.BlockSpec(memory_space=pltpu.HBM)
    total = SPINS * count
    width = halves * COLOURS * LANES
    parts, notes = pl.pallas_call(
        partial(partial_kernel, count, order, loop_scale),
        out_shape=(
            jax.ShapeDtypeStruct((owners * chunk, LANES), jnp.float32),
            jax.ShapeDtypeStruct((8, LANES), jnp.float32),
        ),
        in_specs=[hbm, hbm, hbm],
        out_specs=(vmem, vmem),
        scratch_shapes=[
            pltpu.SMEM(gamma_ids.shape, jnp.int32),
            pltpu.VMEM((1, count), jnp.int32),
            pltpu.VMEM(block.shape, block.dtype),
            pltpu.VMEM(block.shape, jnp.float32),
            pltpu.VMEM((total + 16, width), jnp.bfloat16),
            pltpu.VMEM((total, width), jnp.bfloat16),
            pltpu.VMEM((2, 2, 2, total // LANES, 2, rows, LANES), jnp.float32),
            pltpu.VMEM((2, 4, 1, LANES), jnp.float32),
            pltpu.SemaphoreType.DMA((PIECES + 2,)),
        ],
        compiler_params=pltpu.CompilerParams(vmem_limit_bytes=16 << 20),
        name="partial_gram",
    )(*(in_hbm(v) for v in (gamma_ids, dilution.reshape(1, count), block)))
    swapped = lax.all_to_all(
        parts.reshape(owners, chunk, 1, LANES),
        "space",
        0,
        0,
        tiled=True,
        axis_index_groups=[list(order)],
    )
    mine = pl.pallas_call(
        partial(sum_kernel, owners, chunk),
        out_shape=jax.ShapeDtypeStruct((chunk, LANES), jnp.float32),
        in_specs=[vmem],
        out_specs=vmem,
        compiler_params=pltpu.CompilerParams(vmem_limit_bytes=4 << 20),
        name="sum_chunks",
    )(swapped.reshape(owners * chunk, LANES))
    other = lax.ppermute(mine, "tm", [(0, 1), (1, 0)])
    gram, loops = pl.pallas_call(
        partial(finish_kernel, count, gram_scale),
        out_shape=(
            jax.ShapeDtypeStruct((2, count, LANES), jnp.float32),
            jax.ShapeDtypeStruct((2, 2, count), jnp.float32),
        ),
        in_specs=[vmem, vmem, vmem],
        out_specs=(vmem, vmem),
        compiler_params=pltpu.CompilerParams(vmem_limit_bytes=4 << 20),
        name="finish",
    )(notes, mine, other)
    return gram, jnp.transpose(loops, (0, 2, 1))


def general_shards(vectors, dilution, gamma_ids):
    slices, count, halves, comps, sites = vectors.shape
    owners = lax.axis_size("space")
    total_sites = sites * owners
    gram_scale = 1.0 / math.sqrt(48.0 * total_sites)
    loop_scale = 1.0 / math.sqrt(1.0 * total_sites)
    gamma_real, gamma_imag = pick_gammas(gamma_ids)
    spin_pick = ((dilution % 12 // 3)[:, None] == jnp.arange(4, dtype=jnp.int32)[None, :]).astype(
        jnp.float32
    )
    colour_pick = ((dilution % 3)[:, None] == jnp.arange(3, dtype=jnp.int32)[None, :]).astype(
        jnp.float32
    )
    time_class = dilution // 12
    ein = partial(jnp.einsum, precision=highest)
    lowein = partial(jnp.einsum, preferred_element_type=jnp.float32)
    first_slice = lax.axis_index("tm") * slices
    rows_real = ein("gba,ib->gia", gamma_real, spin_pick)
    rows_imag = ein("gba,ib->gia", gamma_imag, spin_pick)

    def one_slice(inputs):
        block, slice_index = inputs
        spinor = block.reshape(count, 2, 4, 3 * sites)
        real_part = spinor[:, 0]
        imag_part = spinor[:, 1]
        pair_real = lowein("iak,jbk->iajb", real_part, real_part) + lowein(
            "iak,jbk->iajb", imag_part, imag_part
        )
        pair_imag = lowein("iak,jbk->iajb", real_part, imag_part) - lowein(
            "iak,jbk->iajb", imag_part, real_part
        )
        gram_real = ein("gab,iajb->gij", gamma_real, pair_real) - ein(
            "gab,iajb->gij", gamma_imag, pair_imag
        )
        gram_imag = ein("gab,iajb->gij", gamma_real, pair_imag) + ein(
            "gab,iajb->gij", gamma_imag, pair_real
        )
        gram = jnp.concatenate([gram_real, gram_imag], axis=2).reshape(-1, 2 * count)
        gram = gram * gram_scale
        site_sums = jnp.sum(block, axis=-1, dtype=jnp.float32).reshape(count, 2, 4, 3)
        picked = ein("ipac,ic->ipa", site_sums, colour_pick)
        loop_real = ein("gia,ia->gi", rows_real, picked[:, 0]) - ein(
            "gia,ia->gi", rows_imag, picked[:, 1]
        )
        loop_imag = ein("gia,ia->gi", rows_real, picked[:, 1]) + ein(
            "gia,ia->gi", rows_imag, picked[:, 0]
        )
        live = (time_class == slice_index % TDIL).astype(jnp.float32)[None, :]
        loops = jnp.stack([loop_real * live, loop_imag * live], axis=-1).reshape(-1, 2) * loop_scale
        return (gram, loops)

    gram_terms, loop_terms = lax.map(
        one_slice, (vectors, first_slice + jnp.arange(slices, dtype=jnp.int32))
    )
    owned = gram_terms.shape[1] // owners
    width = 2 * count
    padded = jnp.pad(loop_terms, ((0, 0), (0, 0), (0, width - 2)))
    terms = jnp.stack([gram_terms, padded], axis=1).reshape(slices * 2, owners, owned, width)
    swapped = lax.all_to_all(terms, "space", 1, 1, tiled=True)
    mine = jnp.sum(swapped, axis=1).reshape(slices, 2, owned, width)
    every = lax.all_gather(mine, "tm", axis=0, tiled=True)
    return (every[:, 0], every[:, 1, :, :2])


def solution(mesh):
    placed = (P("tm", None, None, None, "space"), P(), P())

    def shards(vectors, dilution, gamma_ids):
        slices, count, halves, comps, sites = vectors.shape
        packable = (
            slices == 1
            and mesh.shape["tm"] == 2
            and gamma_ids.shape[0] == mesh.shape["space"]
            and 2 * count == LANES
            and comps == SPINS * COLOURS
            and halves == 2
            and sites == LANES
        )
        body = packed_shards if packable else general_shards
        return body(vectors, dilution, gamma_ids)

    return jax.shard_map(
        shards,
        mesh=mesh,
        in_specs=placed,
        out_specs=(P(None, "space", None), P(None, "space", None)),
        check_vma=False,
    )
```

```python
from functools import partial
import math

import jax
import jax.numpy as jnp
from jax import lax
from jax.experimental import pallas as pl
from jax.experimental.pallas import tpu as pltpu
from jax.sharding import PartitionSpec as P

TDIL = 2
SPINS = 4
COLOURS = 3
LANES = 128

EXCHANGE_ORDERS = (
    (11, 1, 14, 7, 2, 8, 4, 13, 0, 6, 3, 5, 15, 9, 10, 12),
    (9, 8, 0, 10, 15, 4, 1, 3, 5, 2, 11, 12, 6, 7, 13, 14),
)


highest = lax.Precision.HIGHEST


def zero_square():
    return [[0, 0, 0, 0] for _ in range(4)]


def pair_product(left, right):
    real_out = zero_square()
    imag_out = zero_square()
    for row in range(4):
        for col in range(4):
            acc_real = 0
            acc_imag = 0
            for mid in range(4):
                acc_real += (
                    left[0][row][mid] * right[0][mid][col] - left[1][row][mid] * right[1][mid][col]
                )
                acc_imag += (
                    left[0][row][mid] * right[1][mid][col] + left[1][row][mid] * right[0][mid][col]
                )
            real_out[row][col] = acc_real
            imag_out[row][col] = acc_imag
    return (real_out, imag_out)


def dirac_squares():
    factors = [
        (zero_square(), [[0, 0, 0, 1], [0, 0, 1, 0], [0, -1, 0, 0], [-1, 0, 0, 0]]),
        ([[0, 0, 0, -1], [0, 0, 1, 0], [0, 1, 0, 0], [-1, 0, 0, 0]], zero_square()),
        (zero_square(), [[0, 0, 1, 0], [0, 0, 0, -1], [-1, 0, 0, 0], [0, 1, 0, 0]]),
        ([[0, 0, 1, 0], [0, 0, 0, 1], [1, 0, 0, 0], [0, 1, 0, 0]], zero_square()),
    ]
    squares = []
    for number in range(16):
        current = ([[1 if a == b else 0 for b in range(4)] for a in range(4)], zero_square())
        for position in range(4):
            if number >> position & 1:
                current = pair_product(current, factors[position])
        squares.append(current)
    return squares


def dirac_entries():
    entries = []
    for real, imag in dirac_squares():
        mask = next(b for b in range(4) if real[0][b] or imag[0][b])
        imaginary = int(imag[0][mask] != 0)
        square, other = (imag, real) if imaginary else (real, imag)
        values = [square[a][a ^ mask] for a in range(4)]
        assert all(abs(v) == 1 for v in values)
        assert sum(abs(v) for line in square for v in line) == 4
        assert not any(v for line in other for v in line)
        flips = {values[a] * values[a ^ mask] * (-1 if imaginary else 1) for a in range(4)}
        assert len(flips) == 1
        entries.append((imaginary, int(flips == {-1}), mask, tuple(values)))
    return entries


GAMMAS = dirac_entries()
ANTI = sum(entry[1] << number for number, entry in enumerate(GAMMAS))


def pick_gammas(gamma_ids):
    squares = dirac_squares()
    table_real = [[v for line in real for v in line] for real, _ in squares]
    table_imag = [[v for line in imag for v in line] for _, imag in squares]
    choose = (gamma_ids[:, None] == jnp.arange(16, dtype=jnp.int32)[None, :]).astype(jnp.float32)
    gamma_real = jnp.dot(
        choose, jnp.asarray(table_real, dtype=jnp.float32), precision=highest
    ).reshape(-1, 4, 4)
    gamma_imag = jnp.dot(
        choose, jnp.asarray(table_imag, dtype=jnp.float32), precision=highest
    ).reshape(-1, 4, 4)
    return (gamma_real, gamma_imag)


def in_hbm(value):
    return pltpu.with_memory_space_constraint(value, pltpu.HBM)


def half_swap(value, count):
    return pltpu.roll(value, count, 1)


def partial_kernel(
    count, orders, loop_scale, ids_hbm, dilution_hbm, block_hbm, out_ref, notes_ref,
    ids_ref, dilution_ref, block_ref, flat_ref, gram_ref, loop_ref, sems,
):
    comps = SPINS * COLOURS
    rows = count // 2
    total = SPINS * count
    columns = total // LANES
    get_block = pltpu.make_async_copy(block_hbm, block_ref, sems.at[0])
    get_dilution = pltpu.make_async_copy(dilution_hbm, dilution_ref, sems.at[1])
    get_ids = pltpu.make_async_copy(ids_hbm, ids_ref, sems.at[2])
    get_block.start()
    get_dilution.start()
    get_ids.start()

    get_dilution.wait()
    get_ids.wait()
    lane = lax.broadcasted_iota(jnp.int32, (1, LANES), 1)
    high = lane >= count
    half = high.astype(jnp.int32)
    index = jnp.concatenate([dilution_ref[...]] * 2, axis=1)
    spin_of = index % comps // COLOURS
    colour_of = index % COLOURS
    time_class = index // comps
    own = lax.axis_index("tm")
    mine = ids_ref[lax.axis_index("space")]
    anti = (jnp.int32(ANTI) >> mine) & 1
    notes_ref[pl.ds(0, 1), :] = jnp.full((1, LANES), anti, jnp.int32).astype(jnp.float32)
    notes_ref[pl.ds(1, 1), :] = jnp.where(time_class == own % TDIL, loop_scale, 0.0)
    notes_ref[pl.ds(2, 1), :] = jnp.where(time_class == (1 - own) % TDIL, loop_scale, 0.0)
    get_block.wait()

    flat_ref[...] = block_ref[...].astype(jnp.float32)
    row_id = lax.broadcasted_iota(jnp.int32, (16, 2 * LANES), 0)
    real_lanes = lax.broadcasted_iota(jnp.int32, (16, 2 * LANES), 1) < LANES
    both = None
    for colour in range(COLOURS):
        parts = []
        for part in range(2):
            starts = [(spin * COLOURS + colour) * 2 + part for spin in range(SPINS)]
            pieces = [flat_ref[pl.ds(start, count, stride=2 * comps), :] for start in starts]
            parts.append(jnp.concatenate(pieces, axis=0).astype(jnp.bfloat16))
        spinor = jnp.concatenate(parts, axis=1)
        turned = jnp.concatenate([parts[1], -parts[0]], axis=1)
        ones = jnp.where((row_id == colour) & real_lanes, 1.0, 0.0).astype(jnp.bfloat16)
        term = lax.dot_general(
            jnp.concatenate([spinor, ones], axis=0),
            jnp.concatenate([turned, spinor], axis=0),
            (((1,), (1,)), ((), ())),
            preferred_element_type=jnp.float32,
        )
        both = term if both is None else both + term
    imag, real = both[:, :total], both[:, total:]

    sums = []
    for grid in (real, imag):
        for column in range(columns):
            picked = jnp.zeros((1, LANES), jnp.float32)
            for colour in range(COLOURS):
                row = grid[total + colour : total + colour + 1, column * LANES : (column + 1) * LANES]
                picked = jnp.where(colour_of == colour, row, picked)
            sums.append(picked)
    for mask in range(4):
        source = spin_of ^ mask
        found = []
        for part in range(2):
            lower, upper = sums[part * columns], sums[part * columns + 1]
            value = jnp.where(source >= 2, upper, lower)
            value = jnp.where((source & 1) == half, value, 0.0)
            found.append(value + half_swap(value, count))
        turned = (jnp.where(high, found[1], found[0]), jnp.where(high, found[0], -found[1]))
        for number, (imaginary, _, shift, values) in enumerate(GAMMAS):
            if shift == mask:
                sign = jnp.full((1, LANES), float(values[0]), jnp.float32)
                for spin in range(1, SPINS):
                    sign = jnp.where(spin_of == spin, float(values[spin]), sign)
                loop_ref[pl.ds(number, 1), :] = sign * turned[imaginary]

    wide_high = lax.broadcasted_iota(jnp.int32, (rows, LANES), 1) >= count
    tilt = jnp.where(wide_high, -1.0, 1.0)
    for upper in range(2):
        blocks = []
        for pair in range(2):
            column = upper ^ pair
            across = slice(column * LANES, (column + 1) * LANES)
            pieces = []
            for spin in (2 * pair, 2 * pair + 1):
                down = slice(spin * count, (spin + 1) * count)
                r, i = real[down, across], imag[down, across]
                pieces.append((r + i, r - i))
            blocks.append(pieces)
        for low in range(2):
            made = {}

            def part_of(kind, pair, same):
                if (kind, pair) not in made:
                    even, odd = blocks[pair][0][kind], blocks[pair][1][kind]
                    first, second = (odd, even) if low else (even, odd)
                    kept = jnp.where(wide_high, second[rows:], first[:rows])
                    moved = half_swap(jnp.where(wide_high, second[:rows], first[rows:]), count)
                    made[kind, pair] = (kept, moved)
                kept, moved = made[kind, pair]
                if (kind, pair, same) not in made:
                    made[kind, pair, same] = kept + moved if same else tilt * (kept - moved)
                return made[kind, pair, same]

            for number, (imaginary, anti_one, shift, values) in enumerate(GAMMAS):
                if shift != low + 2 * upper:
                    continue
                kind = imaginary ^ anti_one
                turn = -1 if anti_one and not imaginary else 1
                terms = []
                for pair in range(2):
                    first = turn * values[2 * pair + low]
                    second = turn * values[2 * pair + 1 - low]
                    terms.append((first, part_of(kind, pair, first == second)))
                (one, left), (two, right) = terms
                if one > 0:
                    value = left + right if two > 0 else left - right
                else:
                    value = right - left if two > 0 else -(left + right)
                gram_ref[number] = value

    for place, owners in enumerate(zip(*orders)):
        number = ids_ref[jnp.where(own == 0, *owners)]
        base = place * (rows + 1)
        out_ref[pl.ds(base, rows), :] = gram_ref[number]
        out_ref[pl.ds(base + rows, 1), :] = loop_ref[pl.ds(number, 1), :]


def sum_kernel(chunks, rows, parts_ref, out_ref):
    total = parts_ref[pl.ds(0, rows), :]
    for chunk in range(1, chunks):
        total = total + parts_ref[pl.ds(chunk * rows, rows), :]
    out_ref[...] = total


def finish_kernel(count, gram_scale, notes_ref, mine_ref, other_ref, gram_ref, loop_ref):
    rows = count // 2
    own = lax.axis_index("tm")
    anti = notes_ref[pl.ds(0, 1), :] > 0.5
    high = lax.broadcasted_iota(jnp.int32, (rows, LANES), 1) >= count
    full_high = lax.broadcasted_iota(jnp.int32, (count, LANES), 1) >= count
    for place, (ref, slice_index) in enumerate(((mine_ref, own), (other_ref, 1 - own))):
        packed = ref[pl.ds(0, rows), :]
        swapped = half_swap(packed, count)
        square = jnp.concatenate(
            [jnp.where(high, swapped, packed), jnp.where(high, packed, swapped)], axis=0
        )
        turned = jnp.transpose(jnp.concatenate([square, square], axis=0))[:count]
        real = (square + turned) * (0.5 * gram_scale)
        imag = (square - turned) * (0.5 * gram_scale)
        plain = jnp.where(full_high, imag, real)
        rotated = jnp.where(full_high, real, -imag)
        gram_ref[slice_index] = jnp.where(anti, rotated, plain)
        row = ref[pl.ds(rows, 1), :] * notes_ref[pl.ds(1 + place, 1), :]
        both = jnp.concatenate([row, half_swap(row, count)], axis=0)
        loop_ref[slice_index] = both[:, :count]


def packed_shards(vectors, dilution, gamma_ids):
    slices, count, halves, comps, sites = vectors.shape
    owners = lax.axis_size("space")
    total_sites = sites * owners
    gram_scale = 1.0 / math.sqrt(48.0 * total_sites)
    loop_scale = 1.0 / math.sqrt(1.0 * total_sites)
    orders = EXCHANGE_ORDERS
    if any(len(order) != owners for order in orders):
        orders = (tuple(range(owners)),) * 2
    rows = count // 2
    chunk = rows + 1
    block = jnp.transpose(vectors, (0, 1, 3, 2, 4)).reshape(count * comps * halves, sites)
    vmem = pl.BlockSpec(memory_space=pltpu.VMEM)
    hbm = pl.BlockSpec(memory_space=pltpu.HBM)
    parts, notes = pl.pallas_call(
        partial(partial_kernel, count, orders, loop_scale),
        out_shape=(
            jax.ShapeDtypeStruct((owners * chunk, LANES), jnp.float32),
            jax.ShapeDtypeStruct((8, LANES), jnp.float32),
        ),
        in_specs=[hbm, hbm, hbm],
        out_specs=(vmem, vmem),
        scratch_shapes=[
            pltpu.SMEM(gamma_ids.shape, jnp.int32),
            pltpu.VMEM((1, count), jnp.int32),
            pltpu.VMEM(block.shape, block.dtype),
            pltpu.VMEM(block.shape, jnp.float32),
            pltpu.VMEM((len(GAMMAS), rows, LANES), jnp.float32),
            pltpu.VMEM((len(GAMMAS), LANES), jnp.float32),
            pltpu.SemaphoreType.DMA((3,)),
        ],
        compiler_params=pltpu.CompilerParams(vmem_limit_bytes=16 << 20),
        name="partial_gram",
    )(*(in_hbm(v) for v in (gamma_ids, dilution.reshape(1, count), block)))
    swapped = lax.all_to_all(
        parts.reshape(owners, chunk, 1, LANES),
        ("space", "tm"),
        0,
        0,
        tiled=True,
        axis_index_groups=[[2 * owner + core for owner in orders[core]] for core in range(2)],
    )
    mine = pl.pallas_call(
        partial(sum_kernel, owners, chunk),
        out_shape=jax.ShapeDtypeStruct((chunk, LANES), jnp.float32),
        in_specs=[vmem],
        out_specs=vmem,
        compiler_params=pltpu.CompilerParams(vmem_limit_bytes=4 << 20),
        name="sum_chunks",
    )(swapped.reshape(owners * chunk, LANES))
    other = lax.ppermute(mine, "tm", [(0, 1), (1, 0)])
    gram, loops = pl.pallas_call(
        partial(finish_kernel, count, gram_scale),
        out_shape=(
            jax.ShapeDtypeStruct((2, count, LANES), jnp.float32),
            jax.ShapeDtypeStruct((2, 2, count), jnp.float32),
        ),
        in_specs=[vmem, vmem, vmem],
        out_specs=(vmem, vmem),
        compiler_params=pltpu.CompilerParams(vmem_limit_bytes=4 << 20),
        name="finish",
    )(notes, mine, other)
    return gram, jnp.transpose(loops, (0, 2, 1))


def general_shards(vectors, dilution, gamma_ids):
    slices, count, halves, comps, sites = vectors.shape
    owners = lax.axis_size("space")
    total_sites = sites * owners
    gram_scale = 1.0 / math.sqrt(48.0 * total_sites)
    loop_scale = 1.0 / math.sqrt(1.0 * total_sites)
    gamma_real, gamma_imag = pick_gammas(gamma_ids)
    spin_pick = ((dilution % 12 // 3)[:, None] == jnp.arange(4, dtype=jnp.int32)[None, :]).astype(
        jnp.float32
    )
    colour_pick = ((dilution % 3)[:, None] == jnp.arange(3, dtype=jnp.int32)[None, :]).astype(
        jnp.float32
    )
    time_class = dilution // 12
    ein = partial(jnp.einsum, precision=highest)
    lowein = partial(jnp.einsum, preferred_element_type=jnp.float32)
    first_slice = lax.axis_index("tm") * slices
    rows_real = ein("gba,ib->gia", gamma_real, spin_pick)
    rows_imag = ein("gba,ib->gia", gamma_imag, spin_pick)

    def one_slice(inputs):
        block, slice_index = inputs
        spinor = block.reshape(count, 2, 4, 3 * sites)
        real_part = spinor[:, 0]
        imag_part = spinor[:, 1]
        pair_real = lowein("iak,jbk->iajb", real_part, real_part) + lowein(
            "iak,jbk->iajb", imag_part, imag_part
        )
        pair_imag = lowein("iak,jbk->iajb", real_part, imag_part) - lowein(
            "iak,jbk->iajb", imag_part, real_part
        )
        gram_real = ein("gab,iajb->gij", gamma_real, pair_real) - ein(
            "gab,iajb->gij", gamma_imag, pair_imag
        )
        gram_imag = ein("gab,iajb->gij", gamma_real, pair_imag) + ein(
            "gab,iajb->gij", gamma_imag, pair_real
        )
        gram = jnp.concatenate([gram_real, gram_imag], axis=2).reshape(-1, 2 * count)
        gram = gram * gram_scale
        site_sums = jnp.sum(block, axis=-1, dtype=jnp.float32).reshape(count, 2, 4, 3)
        picked = ein("ipac,ic->ipa", site_sums, colour_pick)
        loop_real = ein("gia,ia->gi", rows_real, picked[:, 0]) - ein(
            "gia,ia->gi", rows_imag, picked[:, 1]
        )
        loop_imag = ein("gia,ia->gi", rows_real, picked[:, 1]) + ein(
            "gia,ia->gi", rows_imag, picked[:, 0]
        )
        live = (time_class == slice_index % TDIL).astype(jnp.float32)[None, :]
        loops = jnp.stack([loop_real * live, loop_imag * live], axis=-1).reshape(-1, 2) * loop_scale
        return (gram, loops)

    gram_terms, loop_terms = lax.map(
        one_slice, (vectors, first_slice + jnp.arange(slices, dtype=jnp.int32))
    )
    owned = gram_terms.shape[1] // owners
    width = 2 * count
    padded = jnp.pad(loop_terms, ((0, 0), (0, 0), (0, width - 2)))
    terms = jnp.stack([gram_terms, padded], axis=1).reshape(slices * 2, owners, owned, width)
    swapped = lax.all_to_all(terms, "space", 1, 1, tiled=True)
    mine = jnp.sum(swapped, axis=1).reshape(slices, 2, owned, width)
    every = lax.all_gather(mine, "tm", axis=0, tiled=True)
    return (every[:, 0], every[:, 1, :, :2])


def solution(mesh):
    placed = (P("tm", None, None, None, "space"), P(), P())

    def shards(vectors, dilution, gamma_ids):
        slices, count, halves, comps, sites = vectors.shape
        packable = (
            slices == 1
            and mesh.shape["tm"] == 2
            and gamma_ids.shape[0] == mesh.shape["space"]
            and 2 * count == LANES
            and comps == SPINS * COLOURS
            and halves == 2
            and sites == LANES
        )
        body = packed_shards if packable else general_shards
        return body(vectors, dilution, gamma_ids)

    return jax.shard_map(
        shards,
        mesh=mesh,
        in_specs=placed,
        out_specs=(P(None, "space", None), P(None, "space", None)),
        check_vma=False,
    )
```

```python
from functools import partial
import math

import jax
import jax.numpy as jnp
from jax import lax
from jax.experimental import pallas as pl
from jax.experimental.pallas import tpu as pltpu
from jax.sharding import PartitionSpec as P

TDIL = 2
SPINS = 4
COLOURS = 3
LANES = 128

EXCHANGE_ORDERS = (
    (15, 8, 14, 11, 5, 6, 12, 4, 9, 0, 2, 1, 13, 10, 7, 3),
    (11, 9, 12, 1, 2, 15, 13, 6, 0, 10, 5, 8, 3, 7, 4, 14),
)


highest = lax.Precision.HIGHEST


def zero_square():
    return [[0, 0, 0, 0] for _ in range(4)]


def pair_product(left, right):
    real_out = zero_square()
    imag_out = zero_square()
    for row in range(4):
        for col in range(4):
            acc_real = 0
            acc_imag = 0
            for mid in range(4):
                acc_real += (
                    left[0][row][mid] * right[0][mid][col] - left[1][row][mid] * right[1][mid][col]
                )
                acc_imag += (
                    left[0][row][mid] * right[1][mid][col] + left[1][row][mid] * right[0][mid][col]
                )
            real_out[row][col] = acc_real
            imag_out[row][col] = acc_imag
    return (real_out, imag_out)


def dirac_squares():
    factors = [
        (zero_square(), [[0, 0, 0, 1], [0, 0, 1, 0], [0, -1, 0, 0], [-1, 0, 0, 0]]),
        ([[0, 0, 0, -1], [0, 0, 1, 0], [0, 1, 0, 0], [-1, 0, 0, 0]], zero_square()),
        (zero_square(), [[0, 0, 1, 0], [0, 0, 0, -1], [-1, 0, 0, 0], [0, 1, 0, 0]]),
        ([[0, 0, 1, 0], [0, 0, 0, 1], [1, 0, 0, 0], [0, 1, 0, 0]], zero_square()),
    ]
    squares = []
    for number in range(16):
        current = ([[1 if a == b else 0 for b in range(4)] for a in range(4)], zero_square())
        for position in range(4):
            if number >> position & 1:
                current = pair_product(current, factors[position])
        squares.append(current)
    return squares


def dirac_entries():
    entries = []
    for real, imag in dirac_squares():
        mask = next(b for b in range(4) if real[0][b] or imag[0][b])
        imaginary = int(imag[0][mask] != 0)
        square, other = (imag, real) if imaginary else (real, imag)
        values = [square[a][a ^ mask] for a in range(4)]
        assert all(abs(v) == 1 for v in values)
        assert sum(abs(v) for line in square for v in line) == 4
        assert not any(v for line in other for v in line)
        flips = {values[a] * values[a ^ mask] * (-1 if imaginary else 1) for a in range(4)}
        assert len(flips) == 1
        entries.append((imaginary, int(flips == {-1}), mask, tuple(values)))
    return entries


GAMMAS = dirac_entries()
ANTI = sum(entry[1] << number for number, entry in enumerate(GAMMAS))


def pick_gammas(gamma_ids):
    squares = dirac_squares()
    table_real = [[v for line in real for v in line] for real, _ in squares]
    table_imag = [[v for line in imag for v in line] for _, imag in squares]
    choose = (gamma_ids[:, None] == jnp.arange(16, dtype=jnp.int32)[None, :]).astype(jnp.float32)
    gamma_real = jnp.dot(
        choose, jnp.asarray(table_real, dtype=jnp.float32), precision=highest
    ).reshape(-1, 4, 4)
    gamma_imag = jnp.dot(
        choose, jnp.asarray(table_imag, dtype=jnp.float32), precision=highest
    ).reshape(-1, 4, 4)
    return (gamma_real, gamma_imag)


def in_hbm(value):
    return pltpu.with_memory_space_constraint(value, pltpu.HBM)


def half_swap(value, count):
    return pltpu.roll(value, count, 1)


def partial_kernel(
    count, orders, loop_scale, ids_hbm, dilution_hbm, block_hbm, out_ref, notes_ref,
    ids_ref, dilution_ref, block_ref, flat_ref, gram_ref, loop_ref, sems,
):
    comps = SPINS * COLOURS
    rows = count // 2
    total = SPINS * count
    columns = total // LANES
    get_block = pltpu.make_async_copy(block_hbm, block_ref, sems.at[0])
    get_dilution = pltpu.make_async_copy(dilution_hbm, dilution_ref, sems.at[1])
    get_ids = pltpu.make_async_copy(ids_hbm, ids_ref, sems.at[2])
    get_block.start()
    get_dilution.start()
    get_ids.start()

    get_dilution.wait()
    get_ids.wait()
    lane = lax.broadcasted_iota(jnp.int32, (1, LANES), 1)
    high = lane >= count
    half = high.astype(jnp.int32)
    index = jnp.concatenate([dilution_ref[...]] * 2, axis=1)
    spin_of = index % comps // COLOURS
    colour_of = index % COLOURS
    time_class = index // comps
    own = lax.axis_index("tm")
    mine = ids_ref[lax.axis_index("space")]
    anti = (jnp.int32(ANTI) >> mine) & 1
    notes_ref[pl.ds(0, 1), :] = jnp.full((1, LANES), anti, jnp.int32).astype(jnp.float32)
    notes_ref[pl.ds(1, 1), :] = jnp.where(time_class == own % TDIL, loop_scale, 0.0)
    notes_ref[pl.ds(2, 1), :] = jnp.where(time_class == (1 - own) % TDIL, loop_scale, 0.0)
    get_block.wait()

    flat_ref[...] = block_ref[...].astype(jnp.float32)
    row_id = lax.broadcasted_iota(jnp.int32, (16, 2 * LANES), 0)
    real_lanes = lax.broadcasted_iota(jnp.int32, (16, 2 * LANES), 1) < LANES
    both = None
    for colour in range(COLOURS):
        parts = []
        for part in range(2):
            starts = [(spin * COLOURS + colour) * 2 + part for spin in range(SPINS)]
            pieces = [flat_ref[pl.ds(start, count, stride=2 * comps), :] for start in starts]
            parts.append(jnp.concatenate(pieces, axis=0).astype(jnp.bfloat16))
        spinor = jnp.concatenate(parts, axis=1)
        turned = jnp.concatenate([parts[1], -parts[0]], axis=1)
        ones = jnp.where((row_id == colour) & real_lanes, 1.0, 0.0).astype(jnp.bfloat16)
        term = lax.dot_general(
            jnp.concatenate([spinor, ones], axis=0),
            jnp.concatenate([turned, spinor], axis=0),
            (((1,), (1,)), ((), ())),
            preferred_element_type=jnp.float32,
        )
        both = term if both is None else both + term
    imag, real = both[:, :total], both[:, total:]

    sums = []
    for grid in (real, imag):
        for column in range(columns):
            picked = jnp.zeros((1, LANES), jnp.float32)
            for colour in range(COLOURS):
                row = grid[total + colour : total + colour + 1, column * LANES : (column + 1) * LANES]
                picked = jnp.where(colour_of == colour, row, picked)
            sums.append(picked)
    for mask in range(4):
        source = spin_of ^ mask
        found = []
        for part in range(2):
            lower, upper = sums[part * columns], sums[part * columns + 1]
            value = jnp.where(source >= 2, upper, lower)
            value = jnp.where((source & 1) == half, value, 0.0)
            found.append(value + half_swap(value, count))
        turned = (jnp.where(high, found[1], found[0]), jnp.where(high, found[0], -found[1]))
        for number, (imaginary, _, shift, values) in enumerate(GAMMAS):
            if shift == mask:
                sign = jnp.full((1, LANES), float(values[0]), jnp.float32)
                for spin in range(1, SPINS):
                    sign = jnp.where(spin_of == spin, float(values[spin]), sign)
                loop_ref[pl.ds(number, 1), :] = sign * turned[imaginary]

    wide_high = lax.broadcasted_iota(jnp.int32, (rows, LANES), 1) >= count
    tilt = jnp.where(wide_high, -1.0, 1.0)
    for upper in range(2):
        blocks = []
        for pair in range(2):
            column = upper ^ pair
            across = slice(column * LANES, (column + 1) * LANES)
            pieces = []
            for spin in (2 * pair, 2 * pair + 1):
                down = slice(spin * count, (spin + 1) * count)
                r, i = real[down, across], imag[down, across]
                pieces.append((r + i, r - i))
            blocks.append(pieces)
        for low in range(2):
            made = {}

            def part_of(kind, pair, same):
                if (kind, pair) not in made:
                    even, odd = blocks[pair][0][kind], blocks[pair][1][kind]
                    first, second = (odd, even) if low else (even, odd)
                    kept = jnp.where(wide_high, second[rows:], first[:rows])
                    moved = half_swap(jnp.where(wide_high, second[:rows], first[rows:]), count)
                    made[kind, pair] = (kept, moved)
                kept, moved = made[kind, pair]
                if (kind, pair, same) not in made:
                    made[kind, pair, same] = kept + moved if same else tilt * (kept - moved)
                return made[kind, pair, same]

            for number, (imaginary, anti_one, shift, values) in enumerate(GAMMAS):
                if shift != low + 2 * upper:
                    continue
                kind = imaginary ^ anti_one
                turn = -1 if anti_one and not imaginary else 1
                terms = []
                for pair in range(2):
                    first = turn * values[2 * pair + low]
                    second = turn * values[2 * pair + 1 - low]
                    terms.append((first, part_of(kind, pair, first == second)))
                (one, left), (two, right) = terms
                if one > 0:
                    value = left + right if two > 0 else left - right
                else:
                    value = right - left if two > 0 else -(left + right)
                gram_ref[number] = value

    for place, owners in enumerate(zip(*orders)):
        number = ids_ref[jnp.where(own == 0, *owners)]
        base = place * (rows + 1)
        out_ref[pl.ds(base, rows), :] = gram_ref[number]
        out_ref[pl.ds(base + rows, 1), :] = loop_ref[pl.ds(number, 1), :]


def sum_kernel(chunks, rows, parts_ref, out_ref):
    total = parts_ref[pl.ds(0, rows), :]
    for chunk in range(1, chunks):
        total = total + parts_ref[pl.ds(chunk * rows, rows), :]
    out_ref[...] = total


def finish_kernel(count, gram_scale, notes_ref, mine_ref, other_ref, gram_ref, loop_ref):
    rows = count // 2
    own = lax.axis_index("tm")
    anti = notes_ref[pl.ds(0, 1), :] > 0.5
    high = lax.broadcasted_iota(jnp.int32, (rows, LANES), 1) >= count
    full_high = lax.broadcasted_iota(jnp.int32, (count, LANES), 1) >= count
    for place, (ref, slice_index) in enumerate(((mine_ref, own), (other_ref, 1 - own))):
        packed = ref[pl.ds(0, rows), :]
        swapped = half_swap(packed, count)
        square = jnp.concatenate(
            [jnp.where(high, swapped, packed), jnp.where(high, packed, swapped)], axis=0
        )
        turned = jnp.transpose(jnp.concatenate([square, square], axis=0))[:count]
        real = (square + turned) * (0.5 * gram_scale)
        imag = (square - turned) * (0.5 * gram_scale)
        plain = jnp.where(full_high, imag, real)
        rotated = jnp.where(full_high, real, -imag)
        gram_ref[slice_index] = jnp.where(anti, rotated, plain)
        row = ref[pl.ds(rows, 1), :] * notes_ref[pl.ds(1 + place, 1), :]
        both = jnp.concatenate([row, half_swap(row, count)], axis=0)
        loop_ref[slice_index] = both[:, :count]


def packed_shards(vectors, dilution, gamma_ids):
    slices, count, halves, comps, sites = vectors.shape
    owners = lax.axis_size("space")
    total_sites = sites * owners
    gram_scale = 1.0 / math.sqrt(48.0 * total_sites)
    loop_scale = 1.0 / math.sqrt(1.0 * total_sites)
    orders = EXCHANGE_ORDERS
    if any(len(order) != owners for order in orders):
        orders = (tuple(range(owners)),) * 2
    rows = count // 2
    chunk = rows + 1
    block = jnp.transpose(vectors, (0, 1, 3, 2, 4)).reshape(count * comps * halves, sites)
    vmem = pl.BlockSpec(memory_space=pltpu.VMEM)
    hbm = pl.BlockSpec(memory_space=pltpu.HBM)
    parts, notes = pl.pallas_call(
        partial(partial_kernel, count, orders, loop_scale),
        out_shape=(
            jax.ShapeDtypeStruct((owners * chunk, LANES), jnp.float32),
            jax.ShapeDtypeStruct((8, LANES), jnp.float32),
        ),
        in_specs=[hbm, hbm, hbm],
        out_specs=(vmem, vmem),
        scratch_shapes=[
            pltpu.SMEM(gamma_ids.shape, jnp.int32),
            pltpu.VMEM((1, count), jnp.int32),
            pltpu.VMEM(block.shape, block.dtype),
            pltpu.VMEM(block.shape, jnp.float32),
            pltpu.VMEM((len(GAMMAS), rows, LANES), jnp.float32),
            pltpu.VMEM((len(GAMMAS), LANES), jnp.float32),
            pltpu.SemaphoreType.DMA((3,)),
        ],
        compiler_params=pltpu.CompilerParams(vmem_limit_bytes=16 << 20),
        name="partial_gram",
    )(*(in_hbm(v) for v in (gamma_ids, dilution.reshape(1, count), block)))
    swapped = lax.all_to_all(
        parts.reshape(owners, chunk, 1, LANES),
        ("space", "tm"),
        0,
        0,
        tiled=True,
        axis_index_groups=[[2 * owner + core for owner in orders[core]] for core in range(2)],
    )
    mine = pl.pallas_call(
        partial(sum_kernel, owners, chunk),
        out_shape=jax.ShapeDtypeStruct((chunk, LANES), jnp.float32),
        in_specs=[vmem],
        out_specs=vmem,
        compiler_params=pltpu.CompilerParams(vmem_limit_bytes=4 << 20),
        name="sum_chunks",
    )(swapped.reshape(owners * chunk, LANES))
    other = lax.ppermute(mine, "tm", [(0, 1), (1, 0)])
    gram, loops = pl.pallas_call(
        partial(finish_kernel, count, gram_scale),
        out_shape=(
            jax.ShapeDtypeStruct((2, count, LANES), jnp.float32),
            jax.ShapeDtypeStruct((2, 2, count), jnp.float32),
        ),
        in_specs=[vmem, vmem, vmem],
        out_specs=(vmem, vmem),
        compiler_params=pltpu.CompilerParams(vmem_limit_bytes=4 << 20),
        name="finish",
    )(notes, mine, other)
    return gram, jnp.transpose(loops, (0, 2, 1))


def general_shards(vectors, dilution, gamma_ids):
    slices, count, halves, comps, sites = vectors.shape
    owners = lax.axis_size("space")
    total_sites = sites * owners
    gram_scale = 1.0 / math.sqrt(48.0 * total_sites)
    loop_scale = 1.0 / math.sqrt(1.0 * total_sites)
    gamma_real, gamma_imag = pick_gammas(gamma_ids)
    spin_pick = ((dilution % 12 // 3)[:, None] == jnp.arange(4, dtype=jnp.int32)[None, :]).astype(
        jnp.float32
    )
    colour_pick = ((dilution % 3)[:, None] == jnp.arange(3, dtype=jnp.int32)[None, :]).astype(
        jnp.float32
    )
    time_class = dilution // 12
    ein = partial(jnp.einsum, precision=highest)
    lowein = partial(jnp.einsum, preferred_element_type=jnp.float32)
    first_slice = lax.axis_index("tm") * slices
    rows_real = ein("gba,ib->gia", gamma_real, spin_pick)
    rows_imag = ein("gba,ib->gia", gamma_imag, spin_pick)

    def one_slice(inputs):
        block, slice_index = inputs
        spinor = block.reshape(count, 2, 4, 3 * sites)
        real_part = spinor[:, 0]
        imag_part = spinor[:, 1]
        pair_real = lowein("iak,jbk->iajb", real_part, real_part) + lowein(
            "iak,jbk->iajb", imag_part, imag_part
        )
        pair_imag = lowein("iak,jbk->iajb", real_part, imag_part) - lowein(
            "iak,jbk->iajb", imag_part, real_part
        )
        gram_real = ein("gab,iajb->gij", gamma_real, pair_real) - ein(
            "gab,iajb->gij", gamma_imag, pair_imag
        )
        gram_imag = ein("gab,iajb->gij", gamma_real, pair_imag) + ein(
            "gab,iajb->gij", gamma_imag, pair_real
        )
        gram = jnp.concatenate([gram_real, gram_imag], axis=2).reshape(-1, 2 * count)
        gram = gram * gram_scale
        site_sums = jnp.sum(block, axis=-1, dtype=jnp.float32).reshape(count, 2, 4, 3)
        picked = ein("ipac,ic->ipa", site_sums, colour_pick)
        loop_real = ein("gia,ia->gi", rows_real, picked[:, 0]) - ein(
            "gia,ia->gi", rows_imag, picked[:, 1]
        )
        loop_imag = ein("gia,ia->gi", rows_real, picked[:, 1]) + ein(
            "gia,ia->gi", rows_imag, picked[:, 0]
        )
        live = (time_class == slice_index % TDIL).astype(jnp.float32)[None, :]
        loops = jnp.stack([loop_real * live, loop_imag * live], axis=-1).reshape(-1, 2) * loop_scale
        return (gram, loops)

    gram_terms, loop_terms = lax.map(
        one_slice, (vectors, first_slice + jnp.arange(slices, dtype=jnp.int32))
    )
    owned = gram_terms.shape[1] // owners
    width = 2 * count
    padded = jnp.pad(loop_terms, ((0, 0), (0, 0), (0, width - 2)))
    terms = jnp.stack([gram_terms, padded], axis=1).reshape(slices * 2, owners, owned, width)
    swapped = lax.all_to_all(terms, "space", 1, 1, tiled=True)
    mine = jnp.sum(swapped, axis=1).reshape(slices, 2, owned, width)
    every = lax.all_gather(mine, "tm", axis=0, tiled=True)
    return (every[:, 0], every[:, 1, :, :2])


def solution(mesh):
    placed = (P("tm", None, None, None, "space"), P(), P())

    def shards(vectors, dilution, gamma_ids):
        slices, count, halves, comps, sites = vectors.shape
        packable = (
            slices == 1
            and mesh.shape["tm"] == 2
            and gamma_ids.shape[0] == mesh.shape["space"]
            and 2 * count == LANES
            and comps == SPINS * COLOURS
            and halves == 2
            and sites == LANES
        )
        body = packed_shards if packable else general_shards
        return body(vectors, dilution, gamma_ids)

    return jax.shard_map(
        shards,
        mesh=mesh,
        in_specs=placed,
        out_specs=(P(None, "space", None), P(None, "space", None)),
        check_vma=False,
    )
```

```python
from functools import partial
import math

import jax
import jax.numpy as jnp
from jax import lax
from jax.experimental import pallas as pl
from jax.experimental.pallas import tpu as pltpu
from jax.sharding import PartitionSpec as P

TDIL = 2
SPINS = 4
COLOURS = 3
LANES = 128

EXCHANGE_ORDERS = (
    (13, 8, 14, 11, 5, 6, 15, 4, 9, 0, 2, 1, 12, 10, 7, 3),
    (11, 9, 12, 1, 2, 15, 13, 6, 0, 10, 5, 8, 3, 7, 4, 14),
)


highest = lax.Precision.HIGHEST


def zero_square():
    return [[0, 0, 0, 0] for _ in range(4)]


def pair_product(left, right):
    real_out = zero_square()
    imag_out = zero_square()
    for row in range(4):
        for col in range(4):
            acc_real = 0
            acc_imag = 0
            for mid in range(4):
                acc_real += (
                    left[0][row][mid] * right[0][mid][col] - left[1][row][mid] * right[1][mid][col]
                )
                acc_imag += (
                    left[0][row][mid] * right[1][mid][col] + left[1][row][mid] * right[0][mid][col]
                )
            real_out[row][col] = acc_real
            imag_out[row][col] = acc_imag
    return (real_out, imag_out)


def dirac_squares():
    factors = [
        (zero_square(), [[0, 0, 0, 1], [0, 0, 1, 0], [0, -1, 0, 0], [-1, 0, 0, 0]]),
        ([[0, 0, 0, -1], [0, 0, 1, 0], [0, 1, 0, 0], [-1, 0, 0, 0]], zero_square()),
        (zero_square(), [[0, 0, 1, 0], [0, 0, 0, -1], [-1, 0, 0, 0], [0, 1, 0, 0]]),
        ([[0, 0, 1, 0], [0, 0, 0, 1], [1, 0, 0, 0], [0, 1, 0, 0]], zero_square()),
    ]
    squares = []
    for number in range(16):
        current = ([[1 if a == b else 0 for b in range(4)] for a in range(4)], zero_square())
        for position in range(4):
            if number >> position & 1:
                current = pair_product(current, factors[position])
        squares.append(current)
    return squares


def dirac_entries():
    entries = []
    for real, imag in dirac_squares():
        mask = next(b for b in range(4) if real[0][b] or imag[0][b])
        imaginary = int(imag[0][mask] != 0)
        square, other = (imag, real) if imaginary else (real, imag)
        values = [square[a][a ^ mask] for a in range(4)]
        assert all(abs(v) == 1 for v in values)
        assert sum(abs(v) for line in square for v in line) == 4
        assert not any(v for line in other for v in line)
        flips = {values[a] * values[a ^ mask] * (-1 if imaginary else 1) for a in range(4)}
        assert len(flips) == 1
        entries.append((imaginary, int(flips == {-1}), mask, tuple(values)))
    return entries


GAMMAS = dirac_entries()
ANTI = sum(entry[1] << number for number, entry in enumerate(GAMMAS))
SWAPPED = sum((entry[0] ^ entry[1]) << number for number, entry in enumerate(GAMMAS))


def pick_gammas(gamma_ids):
    squares = dirac_squares()
    table_real = [[v for line in real for v in line] for real, _ in squares]
    table_imag = [[v for line in imag for v in line] for _, imag in squares]
    choose = (gamma_ids[:, None] == jnp.arange(16, dtype=jnp.int32)[None, :]).astype(jnp.float32)
    gamma_real = jnp.dot(
        choose, jnp.asarray(table_real, dtype=jnp.float32), precision=highest
    ).reshape(-1, 4, 4)
    gamma_imag = jnp.dot(
        choose, jnp.asarray(table_imag, dtype=jnp.float32), precision=highest
    ).reshape(-1, 4, 4)
    return (gamma_real, gamma_imag)


def in_hbm(value):
    return pltpu.with_memory_space_constraint(value, pltpu.HBM)


def half_swap(value, count):
    return pltpu.roll(value, count, 1)


def partial_kernel(
    count, orders, loop_scale, ids_hbm, dilution_hbm, block_hbm, out_ref, notes_ref,
    ids_ref, dilution_ref, block_ref, flat_ref, gram_ref, loop_ref, sems,
):
    comps = SPINS * COLOURS
    rows = count // 2
    total = SPINS * count
    columns = total // LANES
    get_block = pltpu.make_async_copy(block_hbm, block_ref, sems.at[0])
    get_dilution = pltpu.make_async_copy(dilution_hbm, dilution_ref, sems.at[1])
    get_ids = pltpu.make_async_copy(ids_hbm, ids_ref, sems.at[2])
    get_block.start()
    get_dilution.start()
    get_ids.start()

    get_dilution.wait()
    get_ids.wait()
    lane = lax.broadcasted_iota(jnp.int32, (1, LANES), 1)
    high = lane >= count
    half = high.astype(jnp.int32)
    index = jnp.concatenate([dilution_ref[...]] * 2, axis=1)
    spin_of = index % comps // COLOURS
    colour_of = index % COLOURS
    time_class = index // comps
    own = lax.axis_index("tm")
    mine = ids_ref[lax.axis_index("space")]
    flags = [(jnp.int32(word) >> mine) & 1 for word in (ANTI, SWAPPED)]
    for row, flag in enumerate(flags):
        notes_ref[pl.ds(row, 1), :] = jnp.full((1, LANES), flag, jnp.int32).astype(jnp.float32)
    notes_ref[pl.ds(2, 1), :] = jnp.where(time_class == own % TDIL, loop_scale, 0.0)
    notes_ref[pl.ds(3, 1), :] = jnp.where(time_class == (1 - own) % TDIL, loop_scale, 0.0)
    get_block.wait()

    flat_ref[...] = block_ref[...].astype(jnp.float32)
    row_id = lax.broadcasted_iota(jnp.int32, (16, 2 * LANES), 0)
    part_id = lax.broadcasted_iota(jnp.int32, (16, 2 * LANES), 1) // LANES
    blank = jnp.zeros((16, 2 * LANES), jnp.bfloat16)
    both = None
    for colour in range(COLOURS):
        parts = []
        for part in range(2):
            starts = [(spin * COLOURS + colour) * 2 + part for spin in range(SPINS)]
            pieces = [flat_ref[pl.ds(start, count, stride=2 * comps), :] for start in starts]
            parts.append(jnp.concatenate(pieces, axis=0).astype(jnp.bfloat16))
        spinor = jnp.concatenate(parts, axis=1)
        turned = jnp.concatenate([parts[1], -parts[0]], axis=1)
        ones = jnp.where(row_id == 2 * colour + part_id, 1.0, 0.0).astype(jnp.bfloat16)
        for below, right in ((ones, spinor), (blank, turned)):
            term = lax.dot_general(
                jnp.concatenate([spinor, below], axis=0),
                right,
                (((1,), (1,)), ((), ())),
                preferred_element_type=jnp.float32,
            )
            both = term if both is None else both + term

    sums = []
    for part in range(2):
        for column in range(columns):
            picked = jnp.zeros((1, LANES), jnp.float32)
            for colour in range(COLOURS):
                place = total + 2 * colour + part
                row = both[place : place + 1, column * LANES : (column + 1) * LANES]
                picked = jnp.where(colour_of == colour, row, picked)
            sums.append(picked)
    for mask in range(4):
        source = spin_of ^ mask
        found = []
        for part in range(2):
            lower, upper = sums[part * columns], sums[part * columns + 1]
            value = jnp.where(source >= 2, upper, lower)
            value = jnp.where((source & 1) == half, value, 0.0)
            found.append(value + half_swap(value, count))
        turned = (jnp.where(high, found[1], found[0]), jnp.where(high, found[0], -found[1]))
        for number, (imaginary, _, shift, values) in enumerate(GAMMAS):
            if shift == mask:
                sign = jnp.full((1, LANES), float(values[0]), jnp.float32)
                for spin in range(1, SPINS):
                    sign = jnp.where(spin_of == spin, float(values[spin]), sign)
                loop_ref[pl.ds(number, 1), :] = sign * turned[imaginary]

    wide_high = lax.broadcasted_iota(jnp.int32, (rows, LANES), 1) >= count
    tilt = jnp.where(wide_high, -1.0, 1.0)
    for upper in range(2):
        for low in range(2):
            made = []
            for pair in range(2):
                column = upper ^ pair
                across = slice(column * LANES, (column + 1) * LANES)
                spins = (2 * pair + low, 2 * pair + 1 - low)
                first, second = (both[spin * count : (spin + 1) * count, across] for spin in spins)
                kept = jnp.where(wide_high, second[rows:], first[:rows])
                moved = half_swap(jnp.where(wide_high, second[:rows], first[rows:]), count)
                made.append((tilt * (kept - moved), kept + moved))
            shift = low + 2 * upper
            for number, (imaginary, anti_one, mask, values) in enumerate(GAMMAS):
                if mask != shift:
                    continue
                flip = shift if imaginary ^ anti_one else 0
                turn = -1 if anti_one and not imaginary else 1
                signs = [turn * values[spin ^ flip] for spin in range(SPINS)]
                terms = []
                for pair in range(2):
                    lead, other = signs[2 * pair + low], signs[2 * pair + 1 - low]
                    terms.append((lead, made[pair][lead == other]))
                (one, left), (two, right) = terms
                if one > 0:
                    value = left + right if two > 0 else left - right
                else:
                    value = right - left if two > 0 else -(left + right)
                gram_ref[number] = value

    for place, owners in enumerate(zip(*orders)):
        number = ids_ref[jnp.where(own == 0, *owners)]
        base = place * (rows + 1)
        out_ref[pl.ds(base, rows), :] = gram_ref[number]
        out_ref[pl.ds(base + rows, 1), :] = loop_ref[pl.ds(number, 1), :]


def sum_kernel(chunks, rows, parts_ref, out_ref):
    total = parts_ref[pl.ds(0, rows), :]
    for chunk in range(1, chunks):
        total = total + parts_ref[pl.ds(chunk * rows, rows), :]
    out_ref[...] = total


def finish_kernel(count, gram_scale, notes_ref, mine_ref, other_ref, gram_ref, loop_ref):
    rows = count // 2
    own = lax.axis_index("tm")
    anti = notes_ref[pl.ds(0, 1), :] > 0.5
    scale = 0.5 * gram_scale
    imag_scale = jnp.where(notes_ref[pl.ds(1, 1), :] > 0.5, -scale, scale)
    high = lax.broadcasted_iota(jnp.int32, (rows, LANES), 1) >= count
    full_high = lax.broadcasted_iota(jnp.int32, (count, LANES), 1) >= count
    for place, (ref, slice_index) in enumerate(((mine_ref, own), (other_ref, 1 - own))):
        packed = ref[pl.ds(0, rows), :]
        swapped = half_swap(packed, count)
        square = jnp.concatenate(
            [jnp.where(high, swapped, packed), jnp.where(high, packed, swapped)], axis=0
        )
        turned = jnp.transpose(jnp.concatenate([square, square], axis=0))[:count]
        real = (square + turned) * scale
        imag = (square - turned) * imag_scale
        plain = jnp.where(full_high, imag, real)
        rotated = jnp.where(full_high, real, -imag)
        gram_ref[slice_index] = jnp.where(anti, rotated, plain)
        row = ref[pl.ds(rows, 1), :] * notes_ref[pl.ds(2 + place, 1), :]
        both = jnp.concatenate([row, half_swap(row, count)], axis=0)
        loop_ref[slice_index] = both[:, :count]


def packed_shards(vectors, dilution, gamma_ids):
    slices, count, halves, comps, sites = vectors.shape
    owners = lax.axis_size("space")
    total_sites = sites * owners
    gram_scale = 1.0 / math.sqrt(48.0 * total_sites)
    loop_scale = 1.0 / math.sqrt(1.0 * total_sites)
    orders = EXCHANGE_ORDERS
    if any(len(order) != owners for order in orders):
        orders = (tuple(range(owners)),) * 2
    rows = count // 2
    chunk = rows + 1
    block = jnp.transpose(vectors, (0, 1, 3, 2, 4)).reshape(count * comps * halves, sites)
    vmem = pl.BlockSpec(memory_space=pltpu.VMEM)
    hbm = pl.BlockSpec(memory_space=pltpu.HBM)
    parts, notes = pl.pallas_call(
        partial(partial_kernel, count, orders, loop_scale),
        out_shape=(
            jax.ShapeDtypeStruct((owners * chunk, LANES), jnp.float32),
            jax.ShapeDtypeStruct((8, LANES), jnp.float32),
        ),
        in_specs=[hbm, hbm, hbm],
        out_specs=(vmem, vmem),
        scratch_shapes=[
            pltpu.SMEM(gamma_ids.shape, jnp.int32),
            pltpu.VMEM((1, count), jnp.int32),
            pltpu.VMEM(block.shape, block.dtype),
            pltpu.VMEM(block.shape, jnp.float32),
            pltpu.VMEM((len(GAMMAS), rows, LANES), jnp.float32),
            pltpu.VMEM((len(GAMMAS), LANES), jnp.float32),
            pltpu.SemaphoreType.DMA((3,)),
        ],
        compiler_params=pltpu.CompilerParams(vmem_limit_bytes=16 << 20),
        name="partial_gram",
    )(*(in_hbm(v) for v in (gamma_ids, dilution.reshape(1, count), block)))
    swapped = lax.all_to_all(
        parts.reshape(owners, chunk, 1, LANES),
        ("space", "tm"),
        0,
        0,
        tiled=True,
        axis_index_groups=[[2 * owner + core for owner in orders[core]] for core in range(2)],
    )
    mine = pl.pallas_call(
        partial(sum_kernel, owners, chunk),
        out_shape=jax.ShapeDtypeStruct((chunk, LANES), jnp.float32),
        in_specs=[vmem],
        out_specs=vmem,
        compiler_params=pltpu.CompilerParams(vmem_limit_bytes=4 << 20),
        name="sum_chunks",
    )(swapped.reshape(owners * chunk, LANES))
    other = lax.ppermute(mine, "tm", [(0, 1), (1, 0)])
    gram, loops = pl.pallas_call(
        partial(finish_kernel, count, gram_scale),
        out_shape=(
            jax.ShapeDtypeStruct((2, count, LANES), jnp.float32),
            jax.ShapeDtypeStruct((2, 2, count), jnp.float32),
        ),
        in_specs=[vmem, vmem, vmem],
        out_specs=(vmem, vmem),
        compiler_params=pltpu.CompilerParams(vmem_limit_bytes=4 << 20),
        name="finish",
    )(notes, mine, other)
    return gram, jnp.transpose(loops, (0, 2, 1))


def general_shards(vectors, dilution, gamma_ids):
    slices, count, halves, comps, sites = vectors.shape
    owners = lax.axis_size("space")
    total_sites = sites * owners
    gram_scale = 1.0 / math.sqrt(48.0 * total_sites)
    loop_scale = 1.0 / math.sqrt(1.0 * total_sites)
    gamma_real, gamma_imag = pick_gammas(gamma_ids)
    spin_pick = ((dilution % 12 // 3)[:, None] == jnp.arange(4, dtype=jnp.int32)[None, :]).astype(
        jnp.float32
    )
    colour_pick = ((dilution % 3)[:, None] == jnp.arange(3, dtype=jnp.int32)[None, :]).astype(
        jnp.float32
    )
    time_class = dilution // 12
    ein = partial(jnp.einsum, precision=highest)
    lowein = partial(jnp.einsum, preferred_element_type=jnp.float32)
    first_slice = lax.axis_index("tm") * slices
    rows_real = ein("gba,ib->gia", gamma_real, spin_pick)
    rows_imag = ein("gba,ib->gia", gamma_imag, spin_pick)

    def one_slice(inputs):
        block, slice_index = inputs
        spinor = block.reshape(count, 2, 4, 3 * sites)
        real_part = spinor[:, 0]
        imag_part = spinor[:, 1]
        pair_real = lowein("iak,jbk->iajb", real_part, real_part) + lowein(
            "iak,jbk->iajb", imag_part, imag_part
        )
        pair_imag = lowein("iak,jbk->iajb", real_part, imag_part) - lowein(
            "iak,jbk->iajb", imag_part, real_part
        )
        gram_real = ein("gab,iajb->gij", gamma_real, pair_real) - ein(
            "gab,iajb->gij", gamma_imag, pair_imag
        )
        gram_imag = ein("gab,iajb->gij", gamma_real, pair_imag) + ein(
            "gab,iajb->gij", gamma_imag, pair_real
        )
        gram = jnp.concatenate([gram_real, gram_imag], axis=2).reshape(-1, 2 * count)
        gram = gram * gram_scale
        site_sums = jnp.sum(block, axis=-1, dtype=jnp.float32).reshape(count, 2, 4, 3)
        picked = ein("ipac,ic->ipa", site_sums, colour_pick)
        loop_real = ein("gia,ia->gi", rows_real, picked[:, 0]) - ein(
            "gia,ia->gi", rows_imag, picked[:, 1]
        )
        loop_imag = ein("gia,ia->gi", rows_real, picked[:, 1]) + ein(
            "gia,ia->gi", rows_imag, picked[:, 0]
        )
        live = (time_class == slice_index % TDIL).astype(jnp.float32)[None, :]
        loops = jnp.stack([loop_real * live, loop_imag * live], axis=-1).reshape(-1, 2) * loop_scale
        return (gram, loops)

    gram_terms, loop_terms = lax.map(
        one_slice, (vectors, first_slice + jnp.arange(slices, dtype=jnp.int32))
    )
    owned = gram_terms.shape[1] // owners
    width = 2 * count
    padded = jnp.pad(loop_terms, ((0, 0), (0, 0), (0, width - 2)))
    terms = jnp.stack([gram_terms, padded], axis=1).reshape(slices * 2, owners, owned, width)
    swapped = lax.all_to_all(terms, "space", 1, 1, tiled=True)
    mine = jnp.sum(swapped, axis=1).reshape(slices, 2, owned, width)
    every = lax.all_gather(mine, "tm", axis=0, tiled=True)
    return (every[:, 0], every[:, 1, :, :2])


def solution(mesh):
    placed = (P("tm", None, None, None, "space"), P(), P())

    def shards(vectors, dilution, gamma_ids):
        slices, count, halves, comps, sites = vectors.shape
        packable = (
            slices == 1
            and mesh.shape["tm"] == 2
            and gamma_ids.shape[0] == mesh.shape["space"]
            and 2 * count == LANES
            and comps == SPINS * COLOURS
            and halves == 2
            and sites == LANES
        )
        body = packed_shards if packable else general_shards
        return body(vectors, dilution, gamma_ids)

    return jax.shard_map(
        shards,
        mesh=mesh,
        in_specs=placed,
        out_specs=(P(None, "space", None), P(None, "space", None)),
        check_vma=False,
    )
```

```python
from functools import partial
import math

import jax
import jax.numpy as jnp
from jax import lax
from jax.experimental import pallas as pl
from jax.experimental.pallas import tpu as pltpu
from jax.sharding import PartitionSpec as P

TDIL = 2
SPINS = 4
COLOURS = 3
LANES = 128

EXCHANGE_ORDERS = (
    (13, 8, 14, 11, 5, 6, 15, 4, 9, 0, 2, 1, 12, 10, 7, 3),
    (11, 9, 6, 4, 12, 15, 13, 2, 0, 10, 5, 8, 3, 7, 1, 14),
)


highest = lax.Precision.HIGHEST


def zero_square():
    return [[0, 0, 0, 0] for _ in range(4)]


def pair_product(left, right):
    real_out = zero_square()
    imag_out = zero_square()
    for row in range(4):
        for col in range(4):
            acc_real = 0
            acc_imag = 0
            for mid in range(4):
                acc_real += (
                    left[0][row][mid] * right[0][mid][col] - left[1][row][mid] * right[1][mid][col]
                )
                acc_imag += (
                    left[0][row][mid] * right[1][mid][col] + left[1][row][mid] * right[0][mid][col]
                )
            real_out[row][col] = acc_real
            imag_out[row][col] = acc_imag
    return (real_out, imag_out)


def dirac_squares():
    factors = [
        (zero_square(), [[0, 0, 0, 1], [0, 0, 1, 0], [0, -1, 0, 0], [-1, 0, 0, 0]]),
        ([[0, 0, 0, -1], [0, 0, 1, 0], [0, 1, 0, 0], [-1, 0, 0, 0]], zero_square()),
        (zero_square(), [[0, 0, 1, 0], [0, 0, 0, -1], [-1, 0, 0, 0], [0, 1, 0, 0]]),
        ([[0, 0, 1, 0], [0, 0, 0, 1], [1, 0, 0, 0], [0, 1, 0, 0]], zero_square()),
    ]
    squares = []
    for number in range(16):
        current = ([[1 if a == b else 0 for b in range(4)] for a in range(4)], zero_square())
        for position in range(4):
            if number >> position & 1:
                current = pair_product(current, factors[position])
        squares.append(current)
    return squares


def dirac_entries():
    entries = []
    for real, imag in dirac_squares():
        mask = next(b for b in range(4) if real[0][b] or imag[0][b])
        imaginary = int(imag[0][mask] != 0)
        square, other = (imag, real) if imaginary else (real, imag)
        values = [square[a][a ^ mask] for a in range(4)]
        assert all(abs(v) == 1 for v in values)
        assert sum(abs(v) for line in square for v in line) == 4
        assert not any(v for line in other for v in line)
        flips = {values[a] * values[a ^ mask] * (-1 if imaginary else 1) for a in range(4)}
        assert len(flips) == 1
        entries.append((imaginary, int(flips == {-1}), mask, tuple(values)))
    return entries


GAMMAS = dirac_entries()
ANTI = sum(entry[1] << number for number, entry in enumerate(GAMMAS))
SWAPPED = sum((entry[0] ^ entry[1]) << number for number, entry in enumerate(GAMMAS))


def pick_gammas(gamma_ids):
    squares = dirac_squares()
    table_real = [[v for line in real for v in line] for real, _ in squares]
    table_imag = [[v for line in imag for v in line] for _, imag in squares]
    choose = (gamma_ids[:, None] == jnp.arange(16, dtype=jnp.int32)[None, :]).astype(jnp.float32)
    gamma_real = jnp.dot(
        choose, jnp.asarray(table_real, dtype=jnp.float32), precision=highest
    ).reshape(-1, 4, 4)
    gamma_imag = jnp.dot(
        choose, jnp.asarray(table_imag, dtype=jnp.float32), precision=highest
    ).reshape(-1, 4, 4)
    return (gamma_real, gamma_imag)


def in_hbm(value):
    return pltpu.with_memory_space_constraint(value, pltpu.HBM)


def half_swap(value, count):
    return pltpu.roll(value, count, 1)


def partial_kernel(
    count, orders, loop_scale, ids_hbm, dilution_hbm, block_hbm, out_ref, notes_ref,
    ids_ref, dilution_ref, block_ref, flat_ref, gram_ref, loop_ref, sems,
):
    comps = SPINS * COLOURS
    rows = count // 2
    total = SPINS * count
    columns = total // LANES
    get_block = pltpu.make_async_copy(block_hbm, block_ref, sems.at[0])
    get_dilution = pltpu.make_async_copy(dilution_hbm, dilution_ref, sems.at[1])
    get_ids = pltpu.make_async_copy(ids_hbm, ids_ref, sems.at[2])
    get_block.start()
    get_dilution.start()
    get_ids.start()

    get_dilution.wait()
    get_ids.wait()
    lane = lax.broadcasted_iota(jnp.int32, (1, LANES), 1)
    high = lane >= count
    half = high.astype(jnp.int32)
    index = jnp.concatenate([dilution_ref[...]] * 2, axis=1)
    spin_of = index % comps // COLOURS
    colour_of = index % COLOURS
    time_class = index // comps
    own = lax.axis_index("tm")
    mine = ids_ref[lax.axis_index("space")]
    flags = [(jnp.int32(word) >> mine) & 1 for word in (ANTI, SWAPPED)]
    for row, flag in enumerate(flags):
        notes_ref[pl.ds(row, 1), :] = jnp.full((1, LANES), flag, jnp.int32).astype(jnp.float32)
    notes_ref[pl.ds(2, 1), :] = jnp.where(time_class == own % TDIL, loop_scale, 0.0)
    notes_ref[pl.ds(3, 1), :] = jnp.where(time_class == (1 - own) % TDIL, loop_scale, 0.0)
    get_block.wait()

    flat_ref[...] = block_ref[...].astype(jnp.float32)
    row_id = lax.broadcasted_iota(jnp.int32, (16, 2 * LANES), 0)
    part_id = lax.broadcasted_iota(jnp.int32, (16, 2 * LANES), 1) // LANES
    blank = jnp.zeros((16, 2 * LANES), jnp.bfloat16)
    both = None
    for colour in range(COLOURS):
        parts = []
        for part in range(2):
            starts = [(spin * COLOURS + colour) * 2 + part for spin in range(SPINS)]
            pieces = [flat_ref[pl.ds(start, count, stride=2 * comps), :] for start in starts]
            parts.append(jnp.concatenate(pieces, axis=0).astype(jnp.bfloat16))
        spinor = jnp.concatenate(parts, axis=1)
        turned = jnp.concatenate([parts[1], -parts[0]], axis=1)
        ones = jnp.where(row_id == 2 * colour + part_id, 1.0, 0.0).astype(jnp.bfloat16)
        for below, right in ((ones, spinor), (blank, turned)):
            term = lax.dot_general(
                jnp.concatenate([spinor, below], axis=0),
                right,
                (((1,), (1,)), ((), ())),
                preferred_element_type=jnp.float32,
            )
            both = term if both is None else both + term

    sums = []
    for part in range(2):
        for column in range(columns):
            picked = jnp.zeros((1, LANES), jnp.float32)
            for colour in range(COLOURS):
                place = total + 2 * colour + part
                row = both[place : place + 1, column * LANES : (column + 1) * LANES]
                picked = jnp.where(colour_of == colour, row, picked)
            sums.append(picked)
    for mask in range(4):
        source = spin_of ^ mask
        found = []
        for part in range(2):
            lower, upper = sums[part * columns], sums[part * columns + 1]
            value = jnp.where(source >= 2, upper, lower)
            value = jnp.where((source & 1) == half, value, 0.0)
            found.append(value + half_swap(value, count))
        turned = (jnp.where(high, found[1], found[0]), jnp.where(high, found[0], -found[1]))
        for number, (imaginary, _, shift, values) in enumerate(GAMMAS):
            if shift == mask:
                sign = jnp.full((1, LANES), float(values[0]), jnp.float32)
                for spin in range(1, SPINS):
                    sign = jnp.where(spin_of == spin, float(values[spin]), sign)
                loop_ref[pl.ds(number, 1), :] = sign * turned[imaginary]

    wide_high = lax.broadcasted_iota(jnp.int32, (rows, LANES), 1) >= count
    tilt = jnp.where(wide_high, -1.0, 1.0)
    for upper in range(2):
        for low in range(2):
            made = []
            for pair in range(2):
                column = upper ^ pair
                across = slice(column * LANES, (column + 1) * LANES)
                spins = (2 * pair + low, 2 * pair + 1 - low)
                first, second = (both[spin * count : (spin + 1) * count, across] for spin in spins)
                kept = jnp.where(wide_high, second[rows:], first[:rows])
                moved = half_swap(jnp.where(wide_high, second[:rows], first[rows:]), count)
                made.append((tilt * (kept - moved), kept + moved))
            shift = low + 2 * upper
            for number, (imaginary, anti_one, mask, values) in enumerate(GAMMAS):
                if mask != shift:
                    continue
                flip = shift if imaginary ^ anti_one else 0
                turn = -1 if anti_one and not imaginary else 1
                signs = [turn * values[spin ^ flip] for spin in range(SPINS)]
                terms = []
                for pair in range(2):
                    lead, other = signs[2 * pair + low], signs[2 * pair + 1 - low]
                    terms.append((lead, made[pair][lead == other]))
                (one, left), (two, right) = terms
                if one > 0:
                    value = left + right if two > 0 else left - right
                else:
                    value = right - left if two > 0 else -(left + right)
                gram_ref[number] = value

    for place, owners in enumerate(zip(*orders)):
        number = ids_ref[jnp.where(own == 0, *owners)]
        base = place * (rows + 1)
        out_ref[pl.ds(base, rows), :] = gram_ref[number]
        out_ref[pl.ds(base + rows, 1), :] = loop_ref[pl.ds(number, 1), :]


def sum_kernel(chunks, rows, parts_ref, out_ref):
    total = parts_ref[pl.ds(0, rows), :]
    for chunk in range(1, chunks):
        total = total + parts_ref[pl.ds(chunk * rows, rows), :]
    out_ref[...] = total


def finish_kernel(count, gram_scale, notes_ref, mine_ref, other_ref, gram_ref, loop_ref):
    rows = count // 2
    own = lax.axis_index("tm")
    anti = notes_ref[pl.ds(0, 1), :] > 0.5
    scale = 0.5 * gram_scale
    imag_scale = jnp.where(notes_ref[pl.ds(1, 1), :] > 0.5, -scale, scale)
    high = lax.broadcasted_iota(jnp.int32, (rows, LANES), 1) >= count
    full_high = lax.broadcasted_iota(jnp.int32, (count, LANES), 1) >= count
    for place, (ref, slice_index) in enumerate(((mine_ref, own), (other_ref, 1 - own))):
        packed = ref[pl.ds(0, rows), :]
        swapped = half_swap(packed, count)
        square = jnp.concatenate(
            [jnp.where(high, swapped, packed), jnp.where(high, packed, swapped)], axis=0
        )
        turned = jnp.transpose(jnp.concatenate([square, square], axis=0))[:count]
        real = (square + turned) * scale
        imag = (square - turned) * imag_scale
        plain = jnp.where(full_high, imag, real)
        rotated = jnp.where(full_high, real, -imag)
        gram_ref[slice_index] = jnp.where(anti, rotated, plain)
        row = ref[pl.ds(rows, 1), :] * notes_ref[pl.ds(2 + place, 1), :]
        both = jnp.concatenate([row, half_swap(row, count)], axis=0)
        loop_ref[slice_index] = both[:, :count]


def packed_shards(vectors, dilution, gamma_ids):
    slices, count, halves, comps, sites = vectors.shape
    owners = lax.axis_size("space")
    total_sites = sites * owners
    gram_scale = 1.0 / math.sqrt(48.0 * total_sites)
    loop_scale = 1.0 / math.sqrt(1.0 * total_sites)
    orders = EXCHANGE_ORDERS
    if any(len(order) != owners for order in orders):
        orders = (tuple(range(owners)),) * 2
    rows = count // 2
    chunk = rows + 1
    block = jnp.transpose(vectors, (0, 1, 3, 2, 4)).reshape(count * comps * halves, sites)
    vmem = pl.BlockSpec(memory_space=pltpu.VMEM)
    hbm = pl.BlockSpec(memory_space=pltpu.HBM)
    parts, notes = pl.pallas_call(
        partial(partial_kernel, count, orders, loop_scale),
        out_shape=(
            jax.ShapeDtypeStruct((owners * chunk, LANES), jnp.float32),
            jax.ShapeDtypeStruct((8, LANES), jnp.float32),
        ),
        in_specs=[hbm, hbm, hbm],
        out_specs=(vmem, vmem),
        scratch_shapes=[
            pltpu.SMEM(gamma_ids.shape, jnp.int32),
            pltpu.VMEM((1, count), jnp.int32),
            pltpu.VMEM(block.shape, block.dtype),
            pltpu.VMEM(block.shape, jnp.float32),
            pltpu.VMEM((len(GAMMAS), rows, LANES), jnp.float32),
            pltpu.VMEM((len(GAMMAS), LANES), jnp.float32),
            pltpu.SemaphoreType.DMA((3,)),
        ],
        compiler_params=pltpu.CompilerParams(vmem_limit_bytes=16 << 20),
        name="partial_gram",
    )(*(in_hbm(v) for v in (gamma_ids, dilution.reshape(1, count), block)))
    swapped = lax.all_to_all(
        parts.reshape(owners, chunk, 1, LANES),
        ("space", "tm"),
        0,
        0,
        tiled=True,
        axis_index_groups=[[2 * owner + core for owner in orders[core]] for core in range(2)],
    )
    mine = pl.pallas_call(
        partial(sum_kernel, owners, chunk),
        out_shape=jax.ShapeDtypeStruct((chunk, LANES), jnp.float32),
        in_specs=[vmem],
        out_specs=vmem,
        compiler_params=pltpu.CompilerParams(vmem_limit_bytes=4 << 20),
        name="sum_chunks",
    )(swapped.reshape(owners * chunk, LANES))
    other = lax.ppermute(mine, "tm", [(0, 1), (1, 0)])
    gram, loops = pl.pallas_call(
        partial(finish_kernel, count, gram_scale),
        out_shape=(
            jax.ShapeDtypeStruct((2, count, LANES), jnp.float32),
            jax.ShapeDtypeStruct((2, 2, count), jnp.float32),
        ),
        in_specs=[vmem, vmem, vmem],
        out_specs=(vmem, vmem),
        compiler_params=pltpu.CompilerParams(vmem_limit_bytes=4 << 20),
        name="finish",
    )(notes, mine, other)
    return gram, jnp.transpose(loops, (0, 2, 1))


def general_shards(vectors, dilution, gamma_ids):
    slices, count, halves, comps, sites = vectors.shape
    owners = lax.axis_size("space")
    total_sites = sites * owners
    gram_scale = 1.0 / math.sqrt(48.0 * total_sites)
    loop_scale = 1.0 / math.sqrt(1.0 * total_sites)
    gamma_real, gamma_imag = pick_gammas(gamma_ids)
    spin_pick = ((dilution % 12 // 3)[:, None] == jnp.arange(4, dtype=jnp.int32)[None, :]).astype(
        jnp.float32
    )
    colour_pick = ((dilution % 3)[:, None] == jnp.arange(3, dtype=jnp.int32)[None, :]).astype(
        jnp.float32
    )
    time_class = dilution // 12
    ein = partial(jnp.einsum, precision=highest)
    lowein = partial(jnp.einsum, preferred_element_type=jnp.float32)
    first_slice = lax.axis_index("tm") * slices
    rows_real = ein("gba,ib->gia", gamma_real, spin_pick)
    rows_imag = ein("gba,ib->gia", gamma_imag, spin_pick)

    def one_slice(inputs):
        block, slice_index = inputs
        spinor = block.reshape(count, 2, 4, 3 * sites)
        real_part = spinor[:, 0]
        imag_part = spinor[:, 1]
        pair_real = lowein("iak,jbk->iajb", real_part, real_part) + lowein(
            "iak,jbk->iajb", imag_part, imag_part
        )
        pair_imag = lowein("iak,jbk->iajb", real_part, imag_part) - lowein(
            "iak,jbk->iajb", imag_part, real_part
        )
        gram_real = ein("gab,iajb->gij", gamma_real, pair_real) - ein(
            "gab,iajb->gij", gamma_imag, pair_imag
        )
        gram_imag = ein("gab,iajb->gij", gamma_real, pair_imag) + ein(
            "gab,iajb->gij", gamma_imag, pair_real
        )
        gram = jnp.concatenate([gram_real, gram_imag], axis=2).reshape(-1, 2 * count)
        gram = gram * gram_scale
        site_sums = jnp.sum(block, axis=-1, dtype=jnp.float32).reshape(count, 2, 4, 3)
        picked = ein("ipac,ic->ipa", site_sums, colour_pick)
        loop_real = ein("gia,ia->gi", rows_real, picked[:, 0]) - ein(
            "gia,ia->gi", rows_imag, picked[:, 1]
        )
        loop_imag = ein("gia,ia->gi", rows_real, picked[:, 1]) + ein(
            "gia,ia->gi", rows_imag, picked[:, 0]
        )
        live = (time_class == slice_index % TDIL).astype(jnp.float32)[None, :]
        loops = jnp.stack([loop_real * live, loop_imag * live], axis=-1).reshape(-1, 2) * loop_scale
        return (gram, loops)

    gram_terms, loop_terms = lax.map(
        one_slice, (vectors, first_slice + jnp.arange(slices, dtype=jnp.int32))
    )
    owned = gram_terms.shape[1] // owners
    width = 2 * count
    padded = jnp.pad(loop_terms, ((0, 0), (0, 0), (0, width - 2)))
    terms = jnp.stack([gram_terms, padded], axis=1).reshape(slices * 2, owners, owned, width)
    swapped = lax.all_to_all(terms, "space", 1, 1, tiled=True)
    mine = jnp.sum(swapped, axis=1).reshape(slices, 2, owned, width)
    every = lax.all_gather(mine, "tm", axis=0, tiled=True)
    return (every[:, 0], every[:, 1, :, :2])


def solution(mesh):
    placed = (P("tm", None, None, None, "space"), P(), P())

    def shards(vectors, dilution, gamma_ids):
        slices, count, halves, comps, sites = vectors.shape
        packable = (
            slices == 1
            and mesh.shape["tm"] == 2
            and gamma_ids.shape[0] == mesh.shape["space"]
            and 2 * count == LANES
            and comps == SPINS * COLOURS
            and halves == 2
            and sites == LANES
        )
        body = packed_shards if packable else general_shards
        return body(vectors, dilution, gamma_ids)

    return jax.shard_map(
        shards,
        mesh=mesh,
        in_specs=placed,
        out_specs=(P(None, "space", None), P(None, "space", None)),
        check_vma=False,
    )
```
